512 devices in a mesh: section: 8 (over z), expert: 16 (over y, core), dp: 4 (over x).
Axes of the slice: x: 4, y: 8, z: 8, core: 2. Of those that a mesh axis runs over, the one named last changes fastest.
Arguments:
- arrivals: bfloat16 [8, 4096, 2048], P('section', ('expert', 'dp')), may hold values from -6 to 6
- fresh: bfloat16 [1, 4096, 2048], P(None, ('expert', 'dp')), may hold values from -6 to 6
- routes: int32 [8, 2, 4096, 6], P('section', None, ('expert', 'dp')), may hold values from 0 to 63, as said below
- gates: bfloat16 [8, 2, 4096, 6], P('section', None, ('expert', 'dp')), may hold values from 0.099609375 to 1
- cotangent: bfloat16 [8, 2, 4096, 2048], P('section', None, ('expert', 'dp')), may hold values from -0.3125 to 0.3125
- norm_gain: float32 [8, 2048], P('section'), may hold values from 0.5 to 1.5
- w_gate: bfloat16 [8, 5632, 2048], P('section', 'expert', 'dp'), may hold values from -0.125 to 0.125
- w_up: bfloat16 [8, 5632, 2048], P('section', 'expert', 'dp'), may hold values from -0.125 to 0.125
- w_down: bfloat16 [8, 5632, 2048], P('section', 'expert', 'dp'), may hold values from -0.15625 to 0.15625
Outputs:
- layer_out: bfloat16 [8, 2, 4096, 2048], P('section', None, ('expert', 'dp'))
- grad_down: float32 [8, 5632, 2048], P('section', 'expert', 'dp')
The draws below stay inside these ranges and needn't reach their ends.
Inputs may be any that keep to these rules, and one draw needn't show every extreme that they name: `routes`: each token's 6 entries are different expert numbers.
All inputs are finite; a program needn't handle non-finite values.
Results may differ from the reference program's by a relative error of at most 0.0085.
Values may be sent and summed in bfloat16 or wider, within the bound.
A program may use at most 64 MiB of HBM per device.

```python
import jax
import jax.numpy as jnp
from jax import lax

D = 2048
EXPERTS = 64
TOPK = 6
EXP_HID = 1408
SPLIT = 4
CAP = 12
STEPS = 2
TOK_MB = 64
FLIGHT = 4
HID_DEV = 352
LAYERS = 8
FRESH = 1
TOKENS = 4096


def draw_routes(key, part):
    total_rows = LAYERS * STEPS * TOKENS
    groups = LAYERS * STEPS
    blocks = total_rows // TOK_MB
    key_noise, key_hot, key_rank, key_pick, key_boost = jax.random.split(jax.random.fold_in(key, 7), 5)
    column = jnp.arange(EXPERTS, dtype=jnp.int32)
    noise = jax.random.randint(key_noise, (total_rows, EXPERTS), 0, 1 << 20, dtype=jnp.int32)
    scores = noise * EXPERTS + column[None, :]
    hottest = jax.random.randint(key_hot, (groups,), 0, FLIGHT, dtype=jnp.int32)
    hot_rows = jnp.repeat(hottest, TOKENS)
    ranking = jax.random.randint(key_rank, (blocks, TOK_MB), 0, 1 << 20, dtype=jnp.int32) * TOK_MB + jnp.arange(TOK_MB, dtype=jnp.int32)[None, :]
    ordering = jnp.argsort(jnp.argsort(ranking, axis=1), axis=1).reshape(total_rows)
    forced = (ordering < CAP).astype(jnp.int32)
    scores = scores + forced[:, None] * (column[None, :] == hot_rows[:, None]).astype(jnp.int32) * (1 << 28)
    picked = jax.random.randint(key_pick, (total_rows,), 0, FLIGHT, dtype=jnp.int32)
    boosted = (jax.random.randint(key_boost, (total_rows,), 0, 4, dtype=jnp.int32) == 0).astype(jnp.int32)
    scores = scores + boosted[:, None] * (column[None, :] == picked[:, None]).astype(jnp.int32) * (1 << 27)
    top_values, chosen = lax.top_k(scores, TOPK)
    return chosen.astype(jnp.int32).reshape(LAYERS, STEPS, TOKENS, TOPK)


def level_of(own_key, dims, shards, low, largest):
    level = 1.0
    for dim, blocks in shards:
        draws = jax.random.uniform(jax.random.fold_in(jax.random.fold_in(own_key, 6), dim), (blocks,), jnp.float32, low / len(shards), largest / len(shards))
        level = level * jnp.repeat(jnp.exp(draws), dims[dim] // blocks).reshape((-1,) + (1,) * (len(dims) - 1 - dim))
    return level


def gaussian(rng, extent, width, bound, cuts=(), kind=jnp.bfloat16):
    level = level_of(rng, extent, cuts, -0.22, 0.18) if cuts else 1.0
    values = jax.random.normal(rng, extent, jnp.float32) * width * level
    return jnp.minimum(jnp.maximum(values, -bound), bound).astype(kind)


def setup_inputs(seed: int = 0) -> dict:
    seeds = jax.random.split(jax.random.key(seed), 10)
    return {
        "arrivals": gaussian(seeds[0], (LAYERS, TOKENS, D), 1.0, 6.0, ((0, 8), (1, 64))),
        "fresh": gaussian(seeds[1], (FRESH, TOKENS, D), 1.0, 6.0, ((1, 64),)),
        "routes": draw_routes(jax.random.fold_in(seeds[9], 71), 0),
        "gates": jnp.clip(0.099609375 + 0.9003906 * jax.random.uniform(seeds[3], (LAYERS, STEPS, TOKENS, TOPK), jnp.float32) ** level_of(seeds[3], (LAYERS, STEPS, TOKENS, TOPK), ((0, 8), (2, 64)), -0.2, 0.2), 0.099609375, 1.0).astype(jnp.bfloat16),
        "cotangent": gaussian(seeds[4], (LAYERS, STEPS, TOKENS, D), 0.05, 0.3125, ((0, 8), (2, 64))),
        "norm_gain": jnp.clip(1.0 + 0.1 * jax.random.normal(seeds[5], (LAYERS, D), jnp.float32), 0.5, 1.5),
        "w_gate": gaussian(seeds[6], (LAYERS, FLIGHT * EXP_HID, D), D ** -0.5, 0.125, ((0, 8), (1, 16), (2, 4))),
        "w_up": gaussian(seeds[7], (LAYERS, FLIGHT * EXP_HID, D), D ** -0.5, 0.125, ((0, 8), (1, 16), (2, 4))),
        "w_down": gaussian(seeds[8], (LAYERS, FLIGHT * EXP_HID, D), EXP_HID ** -0.5, 0.15625, ((0, 8), (1, 16), (2, 4))),
    }


def rms_normed(values, gains):
    floats = values.astype(jnp.float32)
    scale = lax.rsqrt(lax.optimization_barrier(jnp.mean(floats * floats, axis=-1, keepdims=True)) + 0.5)
    return (floats * scale * gains[None, :]).astype(jnp.bfloat16)

def layer(inputs, routing, weights, cot, gains, gate_rows, up_rows, down_rows):
    highest = lax.Precision.HIGHEST
    blocks = TOKENS // TOK_MB
    normed = rms_normed(inputs, gains).astype(jnp.float32).reshape(blocks, TOK_MB, D)
    cot_blocks = cot.astype(jnp.float32).reshape(blocks, TOK_MB, D)
    route_blocks = routing.reshape(blocks, TOK_MB, TOPK)
    weight_blocks = weights.astype(jnp.float32).reshape(blocks, TOK_MB, TOPK)
    slot_ids = jnp.arange(CAP, dtype=jnp.int32)
    mixture = jnp.zeros((blocks, TOK_MB, D), jnp.float32)
    grads = []
    for expert in range(FLIGHT):
        matches = route_blocks == expert
        naming = jnp.any(matches, axis=-1).astype(jnp.int32)
        shares = lax.optimization_barrier(jnp.sum(jnp.where(matches, weight_blocks, 0.0), axis=-1))
        places = jnp.cumsum(naming, axis=1) - naming
        select = ((naming[:, None, :] == 1) & (places[:, None, :] == slot_ids[None, :, None])).astype(jnp.float32)
        rows_tok = jnp.einsum('bpt,btd->bpd', select, normed, precision=highest).reshape(blocks * CAP, D)
        rows_cot = jnp.einsum('bpt,btd->bpd', select, cot_blocks, precision=highest).reshape(blocks * CAP, D)
        rows_gate = jnp.einsum('bpt,bt->bp', select, shares, precision=highest)
        first_row = expert * EXP_HID
        gate_w = gate_rows[first_row:first_row + EXP_HID].astype(jnp.float32)
        up_w = up_rows[first_row:first_row + EXP_HID].astype(jnp.float32)
        down_w = down_rows[first_row:first_row + EXP_HID].astype(jnp.float32)
        gate_act = jnp.dot(rows_tok, gate_w.T, precision=highest)
        up_act = jnp.dot(rows_tok, up_w.T, precision=highest)
        hidden = lax.optimization_barrier((jax.nn.silu(gate_act) * up_act).astype(jnp.bfloat16)).astype(jnp.float32)
        pieces = jnp.einsum('rmf,mfd->rmd', hidden.reshape(blocks * CAP, SPLIT, HID_DEV), down_w.reshape(SPLIT, HID_DEV, D), precision=highest)
        pieces = lax.optimization_barrier(pieces.astype(jnp.bfloat16)).astype(jnp.float32)
        expert_out = lax.optimization_barrier(jnp.sum(pieces, axis=1)).reshape(blocks, CAP, D)
        mixture = mixture + jnp.einsum('bpt,bp,bpd->btd', select, rows_gate, expert_out, precision=highest)
        gate_flat = rows_gate.reshape(blocks * CAP)
        weighted = lax.optimization_barrier((hidden * gate_flat[:, None]).astype(jnp.bfloat16)).astype(jnp.float32)
        grads.append(jnp.dot(weighted.T, rows_cot, precision=highest))
    result = (inputs.astype(jnp.float32) + mixture.reshape(TOKENS, D)).astype(jnp.bfloat16)
    return (result, jnp.concatenate(grads, axis=0))

def reference(arrivals, fresh, routes, gates, cotangent, norm_gain, w_gate, w_up, w_down):
    results = []
    grads = []
    for layer_num in range(LAYERS):
        row_out = []
        total = jnp.zeros((FLIGHT * EXP_HID, D), jnp.float32)
        for turn_num in range(STEPS):
            if turn_num == 0:
                inputs = arrivals[layer_num]
            elif layer_num == 0:
                inputs = fresh[turn_num - 1]
            else:
                inputs = results[layer_num - 1][turn_num - 1]
            output, grad_part = layer(inputs, routes[layer_num, turn_num], gates[layer_num, turn_num], cotangent[layer_num, turn_num], norm_gain[layer_num], w_gate[layer_num], w_up[layer_num], w_down[layer_num])
            row_out.append(output)
            total = total + grad_part
        results.append(row_out)
        grads.append(total)
    layer_out = jnp.stack([jnp.stack(row_out) for row_out in results])
    grad_down = jnp.stack(grads)
    return (layer_out, grad_down)
```

```python
import functools

import jax
import jax.numpy as jnp
from jax import lax
from jax.experimental import pallas as pl
from jax.experimental.pallas import tpu as pltpu
from jax.sharding import PartitionSpec as P

SPLIT = 4
CAP = 12
SLOTS = 16
CORES = 2
PAIRS = SPLIT // CORES
MESH = pl.DeviceIdType.MESH
BF = jnp.bfloat16
F32 = jnp.float32

TOK, COT, CROSS, SWAP, HID, RET, PICK, BASE, BACK, SEMS = 0, 5, 7, 9, 11, 13, 21, 22, 23, 24


def mm(a, b, ca=1, cb=0):
    return lax.dot_general(a, b, (((ca,), (cb,)), ((), ())), preferred_element_type=F32)


def kernel(
    n_s, n_e, n_d, steps,
    arr_h, fresh_h, routes_h, gates_h, cot_h, gain_h, wg_h, wu_h, wd_h,
    out, grad,
    wg, wu, wd, routes, gates, gain, cot, fresh, inc, base,
    toks, tokr, cots, cotr, cotx, xg, acc, hid_s, hidr, hp, rets, retr,
    pick_s, pick_r, back, out_v, grad_v,
    load_sems, store_sems, w_send, w_recv, send_sems, recv_sems,
):
    sec = lax.axis_index("section")
    exp = lax.axis_index("expert")
    dp = lax.axis_index("dp")
    n_y = n_e // CORES
    flight = n_e // SPLIT
    rows, cols = inc.shape[2:]
    half = cols // 2
    units = wd.shape[2]
    part_units = units // 2
    width = cols * n_d
    used = flight * SLOTS
    core = lax.rem(exp, CORES)
    y = exp // CORES
    sibling = (sec, exp + 1 - 2 * core, dp)
    nxt = lax.rem(sec + 1, n_s)
    prv = lax.rem(sec + n_s - 1, n_s)
    right = lax.rem(dp + 1, n_d)
    left = lax.rem(dp + n_d - 1, n_d)
    opp = lax.rem(dp + 2, n_d)
    to_right = (sec, exp, right)
    to_left = (sec, exp, left)
    offs = sorted(range(1, n_y), key=lambda o: -min(o, n_y - o))
    last = steps - 1

    def row(o):
        return lax.rem(y + o, n_y)

    barrier = pltpu.get_barrier_semaphore()

    def signal(target):
        pl.semaphore_signal(barrier, inc=1, device_id=target, device_id_type=MESH)

    greet = [(sec, exp, right), (sec, exp, left), sibling, (sec, exp, opp)]
    greet += [(sec, exp + 1 - 2 * core, x) for x in (right, left, opp)]
    greet += [(sec, row(o) * CORES + core, dp) for o in offs]
    greet += [(prv, row(o) * CORES + core, dp) for o in offs + [0]]
    greet += [(nxt, exp, dp)]
    for target in greet:
        signal(target)

    loads = []

    def load(src, dst):
        copy = pltpu.make_async_copy(src, dst, load_sems.at[len(loads)])
        copy.start()
        loads.append(copy)
        return copy

    load_w = [load(wg_h.at[0], wg.at[core, dp]), load(wu_h.at[0], wu.at[core, dp])]
    load_r = [load(routes_h, routes), load(gates_h, gates)]
    load_a = [load(arr_h.at[0, :, pl.ds(d * cols, cols)], inc.at[0, d]) for d in range(n_d)]
    load_w.append(load(wd_h.at[0], wd.at[core, dp]))
    load_c = load(cot_h, cot)
    load_g = [load(gain_h.at[:, pl.ds(d * cols, cols)], gain.at[d]) for d in range(n_d)]
    load_f = [load(fresh_h.at[0, :, pl.ds(d * cols, cols)], fresh.at[d]) for d in range(n_d)]

    def remote(src, dst, sem, target):
        return pltpu.make_async_remote_copy(
            src_ref=src, dst_ref=dst, send_sem=send_sems.at[sem], recv_sem=recv_sems.at[sem],
            device_id=target, device_id_type=MESH,
        )

    def got(ref, sem):
        remote(ref, ref, sem, sibling).wait_recv()

    def sent(ref, sem):
        remote(ref, ref, sem, sibling).wait_send()

    mats = (wg, wu, wd)

    def w_copy(ref, m, i, target):
        return pltpu.make_async_remote_copy(
            src_ref=ref, dst_ref=ref, send_sem=w_send.at[m, i], recv_sem=w_recv.at[m, i],
            device_id=target, device_id_type=MESH,
        )

    def w_own(m):
        load_w[m].wait()
        mine = mats[m].at[core, dp]
        w_copy(mine, m, 0, to_right).start()
        w_copy(mine, m, 1, to_left).start()
        w_copy(mine, m, 4, sibling).start()

    def w_pass(m):
        w = mats[m]
        w_copy(w.at[core, left], m, 0, sibling).wait_recv()
        w_copy(w.at[core, left, pl.ds(0, part_units)], m, 2, to_right).start()
        w_copy(w.at[core, left], m, 5, sibling).start()
        w_copy(w.at[core, right], m, 1, sibling).wait_recv()
        w_copy(w.at[core, right, pl.ds(part_units, part_units)], m, 3, to_left).start()
        w_copy(w.at[core, right], m, 6, sibling).start()

    def w_last(m):
        w = mats[m]
        w_copy(w.at[core, opp, pl.ds(0, part_units)], m, 2, sibling).wait_recv()
        w_copy(w.at[core, opp, pl.ds(part_units, part_units)], m, 3, sibling).wait_recv()
        w_copy(w.at[core, opp], m, 7, sibling).start()

    def w_twin(m, i):
        w_copy(mats[m].at[1 - core, (dp, left, right, opp)[i]], m, 4 + i, sibling).wait_recv()

    lane = lax.broadcasted_iota(jnp.int32, (used, rows), 0)
    lane_expert = lane >> 4
    lane_slot = lane & (SLOTS - 1)
    t_row = lax.broadcasted_iota(jnp.int32, (rows, rows), 0)
    t_col = lax.broadcasted_iota(jnp.int32, (rows, rows), 1)
    earlier_tok = jnp.where(t_row < t_col, 1.0, 0.0).astype(BF)

    def selection(k):
        naming = jnp.zeros((used, rows), F32)
        shares = jnp.zeros((used, rows), F32)
        for j in range(routes.shape[1]):
            hit = routes[0, j, k:k + 1, :] == lane_expert
            naming = jnp.where(hit, 1.0, naming)
            shares = shares + jnp.where(hit, gates[0, j].astype(F32)[k:k + 1, :], 0.0)
        places = mm(naming.astype(BF), earlier_tok)
        chosen = jnp.where(places == lane_slot.astype(F32), naming, 0.0)
        chosen = jnp.where(lane_slot < CAP, chosen, 0.0)
        return chosen.astype(BF), (chosen * shares).astype(BF)

    r_i = lax.broadcasted_iota(jnp.int32, (CAP * n_y, 8 * n_y), 0)
    c_i = lax.broadcasted_iota(jnp.int32, (CAP * n_y, 8 * n_y), 1)
    c_slot = c_i & 7
    shift = r_i - (c_i >> 3) * CAP - c_slot
    low_rows = jnp.where(shift == 0, 1.0, 0.0)
    tail_a = jnp.where((shift == 8) & (c_slot < 4), 1.0, 0.0)
    tail_b = jnp.where((shift == 4) & (c_slot >= 4), 1.0, 0.0)
    map_a = jnp.concatenate([low_rows, tail_a], axis=1).astype(BF)
    map_b = jnp.concatenate([low_rows, tail_b], axis=1).astype(BF)

    def swap(block):
        return jnp.concatenate([block[4:], block[:4]], axis=0)

    def fill(store, k, ch, block):
        for f in range(flight):
            top = block[f * SLOTS:f * SLOTS + 8]
            bottom = block[f * SLOTS + 8:(f + 1) * SLOTS]
            store[k, ch, f, :, :cols] = top.astype(BF)
            store[k, ch, f, :, cols:] = (bottom[:, :half] + swap(bottom[:, half:])).astype(BF)

    def unpack(flat):
        tail = flat[:, cols:]
        return jnp.concatenate(
            [
                mm(map_a, jnp.concatenate([flat[:, :half], tail], axis=0)),
                mm(map_b, jnp.concatenate([flat[:, half:cols], tail], axis=0)),
            ],
            axis=1,
        )

    def flat_of(landing, *at):
        return landing[at].reshape(n_y * 8, cols + half)

    def spread_all(store, landing, k, sem):
        for o in offs:
            remote(
                store.at[k, pl.ds(0, n_d), row(o) // PAIRS],
                landing.at[k, pl.ds(0, n_d), y], sem, (sec, row(o) * CORES + core, dp),
            ).start()
        for d in range(n_d):
            landing[k, d, y] = store[k, d, y // PAIRS]

    def spread_one(store, landing, k, ch, sem):
        for o in offs:
            remote(
                store.at[k, ch, row(o) // PAIRS], landing.at[k, ch, y], sem,
                (sec, row(o) * CORES + core, dp),
            ).start()
        landing[k, ch, y] = store[k, ch, y // PAIRS]

    def prepare(k, ch):
        block = unpack(flat_of(tokr, k, ch))
        xg[ch] = (block * gain[ch]).astype(BF)
        return jnp.sum(block * block, axis=1, keepdims=True)

    def contract(chs, first):
        for i, w in enumerate((wg, wu)):
            for c in range(CORES):
                total = sum(mm(xg[ch], w[c, ch], 1, 1) for ch in chs)
                acc[i, c] = total if first else acc[i, c] + total

    def activate(k, squares):
        scale = lax.rsqrt(squares * (1.0 / width) + 0.5)
        for c in range(CORES):
            act_g = acc[0, c] * scale
            hidden = (act_g / (1.0 + jnp.exp(-act_g)) * (acc[1, c] * scale)).astype(BF)
            hid_s[k, c] = hidden
            hp[0, c] = mm(map_a, hidden, 0, 0).astype(BF)
            hp[1, c] = mm(map_b, hidden, 0, 0).astype(BF)

    def send_hidden(k):
        slot = hidr.at[k, core * n_d + dp]
        for x in (opp, right, left):
            for c in range(CORES):
                there = y * CORES + c
                remote(hid_s.at[k, c], slot, HID + k, (sec, there, x)).start()
        remote(hid_s.at[k, 1 - core], slot, HID + k, sibling).start()
        hidr[k, core * n_d + dp] = hid_s[k, core]

    n_low = 8 * n_y

    def down(k, ch, i):
        a = sum(mm(hp[0, c], wd[c, ch, :, :half]) for c in range(CORES))
        b = sum(mm(hp[1, c], wd[c, ch, :, half:]) for c in range(CORES))
        rets[k, ch, :, :, :half] = a[:n_low].astype(BF).reshape(n_y, 8, half)
        rets[k, ch, :, :, half:cols] = b[:n_low].astype(BF).reshape(n_y, 8, half)
        rets[k, ch, :, :, cols:] = (a[n_low:] + b[n_low:]).astype(BF).reshape(n_y, 8, half)
        there = sec if k == last else nxt
        for o in offs + ([] if k == last else [0]):
            remote(
                rets.at[k, ch, row(o)], retr.at[k, ch, y], RET + k * n_d + i,
                (there, row(o) * CORES + core, dp),
            ).start()
        if k == last:
            retr[k, ch, y] = rets[k, ch, y]

    row_8 = lax.broadcasted_iota(jnp.int32, (8, half), 0)

    def combine(k, ch, i, weights, inputs):
        got(retr.at[k, ch, pl.ds(0, n_y - 1 if k == last else n_y)], RET + k * n_d + i)
        tops = []
        for f in range(flight):
            total = sum(retr[k, ch, f * PAIRS + p].astype(F32) for p in range(PAIRS))
            tail = total[:, cols:]
            tops.append(total[:, :cols])
            tops.append(jnp.concatenate(
                [jnp.where(row_8 < 4, tail, 0.0), jnp.where(row_8 < 4, swap(tail), 0.0)], axis=1
            ))
        mixed = jnp.concatenate(tops, axis=0)
        high = mixed.astype(BF)
        low = (mixed - high.astype(F32)).astype(BF)
        mixture = mm(weights, high, 0, 0) + mm(weights, low, 0, 0)
        return (inputs.astype(F32) + mixture).astype(BF)

    def at_cols(ch):
        return pl.ds(pl.multiple_of(ch * cols, cols), cols)

    pl.semaphore_wait(barrier, len(greet))
    w_own(0)
    w_own(1)
    for copy in load_a:
        copy.wait()
    remote(inc.at[0], base, BASE, (nxt, exp, dp)).start()
    for copy in load_r:
        copy.wait()
    picks = [selection(0)]
    pick_s[...] = picks[0][1]
    remote(pick_s, pick_r, PICK, (nxt, exp, dp)).start()
    for d in range(n_d):
        fill(toks, 0, d, mm(picks[0][0], inc[0, d]))
    spread_all(toks, tokr, 0, TOK)
    picks.append(selection(1))
    load_c.wait()
    for k in range(steps):
        for d in range(n_d):
            fill(cots, k, d, mm(picks[k][1], cot[0, k, :, d * cols:(d + 1) * cols]))
        spread_all(cots, cotr, k, COT + k)
    for copy in load_g + load_f:
        copy.wait()

    w_pass(0)
    got(tokr.at[0, pl.ds(0, n_d), pl.ds(0, n_y - 1)], TOK)
    squares = sum(prepare(0, d) for d in range(n_d))
    w_pass(1)
    w_own(2)
    for m in range(2):
        for i in range(3):
            w_twin(m, i)
    contract((dp, right, left), True)
    w_last(0)
    w_last(1)
    w_twin(0, 3)
    w_twin(1, 3)
    contract((opp,), False)
    activate(0, squares)
    w_twin(2, 0)
    down(0, dp, 0)
    w_pass(2)
    send_hidden(0)
    w_twin(2, 1)
    w_twin(2, 2)
    down(0, right, 1)
    down(0, left, 2)
    for k in range(steps):
        got(cotr.at[k, pl.ds(0, n_d), pl.ds(0, n_y - 1)], COT + k)
        for x in (opp, right, left):
            remote(cotr.at[k, x], cotx.at[k, core, dp], CROSS + k, (sec, exp, x)).start()
        cotx[k, core, dp] = cotr[k, dp]

    def relay(ch, i):
        result = combine(0, ch, i, pick_r[...], base[ch])
        back[ch] = result
        remote(back.at[ch], out.at[0, 0, :, at_cols(ch)], BACK, (prv, exp, dp)).start()
        follow = jnp.where(sec == 0, fresh[ch].astype(F32), result.astype(F32)).astype(BF)
        inc[1, ch] = follow
        fill(toks, 1, ch, mm(picks[1][0], follow))
        spread_one(toks, tokr, 1, ch, TOK + 1 + i)

    def tok_in(ch, i):
        got(tokr.at[1, ch, pl.ds(0, n_y - 1)], TOK + 1 + i)
        return prepare(1, ch)

    got(base, BASE)
    got(pick_r, PICK)
    relay(dp, 0)
    w_last(2)
    w_twin(2, 3)
    down(0, opp, 3)
    relay(right, 1)
    relay(left, 2)
    squares = tok_in(dp, 0)
    contract((dp,), True)
    relay(opp, 3)
    squares = squares + tok_in(right, 1) + tok_in(left, 2)
    contract((right, left), False)
    squares = squares + tok_in(opp, 3)
    contract((opp,), False)
    activate(1, squares)
    order = (dp, right, left, opp)
    for i, ch in enumerate(order):
        down(1, ch, i)
    send_hidden(1)
    for k in range(steps):
        got(cotx.at[k, core, pl.ds(0, n_d - 1)], CROSS + k)
        remote(cotx.at[k, core], cotx.at[k, core], SWAP + k, sibling).start()
    total = None
    for k in range(steps):
        got(cotx.at[k, 0], SWAP + k)
        got(hidr.at[k, pl.ds(0, CORES * n_d - 1)], HID + k)
    for k in range(steps):
        for c in range(CORES):
            rows_cot = jnp.concatenate(
                [unpack(flat_of(cotx, k, c, x)).astype(BF) for x in range(n_d)], axis=0
            )
            rows_hid = hidr[k, pl.ds(c * n_d, n_d)].reshape(n_d * CAP * n_y, units)
            part = mm(rows_hid, rows_cot, 0, 0)
            total = part if total is None else total + part
    grad_v[...] = total
    save_g = pltpu.make_async_copy(grad_v, grad.at[0], store_sems.at[n_d])
    save_g.start()
    saves = [save_g]
    for i, ch in enumerate(order):
        out_v[ch] = combine(1, ch, i, picks[1][1], inc[1, ch])
        save = pltpu.make_async_copy(out_v.at[ch], out.at[0, 1, :, at_cols(ch)], store_sems.at[i])
        save.start()
        saves.append(save)

    got(back, BACK)
    for m in range(3):
        w = mats[m]
        for i in (0, 1, 4, 5, 6, 7):
            w_copy(w.at[0, 0], m, i, sibling).wait_send()
        for i in (2, 3):
            w_copy(w.at[0, 0, pl.ds(0, part_units)], m, i, sibling).wait_send()
    sent(tokr.at[0, pl.ds(0, n_d), pl.ds(0, n_y - 1)], TOK)
    for i in range(n_d):
        sent(tokr.at[1, 0, pl.ds(0, n_y - 1)], TOK + 1 + i)
        sent(rets.at[0, 0], RET + i)
        sent(rets.at[1, 0, pl.ds(0, n_y - 1)], RET + n_d + i)
    for k in range(steps):
        sent(cotr.at[k, pl.ds(0, n_d), pl.ds(0, n_y - 1)], COT + k)
        sent(cotx.at[k, 0, pl.ds(0, n_d - 1)], CROSS + k)
        sent(cotx.at[k, 0], SWAP + k)
        sent(hidr.at[k, pl.ds(0, CORES * n_d - 1)], HID + k)
    sent(pick_s, PICK)
    sent(base, BASE)
    sent(back, BACK)
    for save in saves:
        save.wait()


def finish(out_in, grad_in, out, grad, out_v, grad_v, in_sems, out_sems):
    steps, tok_rows = out_v.shape[1:3]
    units = grad_v.shape[1]
    moves = []
    for k in range(steps):
        for h in range(2):
            part = (0, k, pl.ds(h * tok_rows // 2, tok_rows // 2))
            moves.append((out_in.at[part], out_v.at[part], out.at[part]))
    for h in range(4):
        part = (0, pl.ds(h * units // 4, units // 4))
        moves.append((grad_in.at[part], grad_v.at[part], grad.at[part]))
    loads = [
        pltpu.make_async_copy(src, held, in_sems.at[i]) for i, (src, held, _) in enumerate(moves)
    ]
    stores = [
        pltpu.make_async_copy(held, dst, out_sems.at[i]) for i, (_, held, dst) in enumerate(moves)
    ]
    for load in loads:
        load.start()
    for load, store in zip(loads, stores):
        load.wait()
        store.start()
    for store in stores:
        store.wait()


def local(sizes, arrivals, fresh, routes, gates, cotangent, norm_gain, w_gate, w_up, w_down):
    n_s, n_e, n_d = sizes
    steps = routes.shape[1]
    tok_rows, width = arrivals.shape[1:]
    units, cols = w_gate.shape[1:]
    flight = n_e // SPLIT
    n_y = n_e // CORES
    rows = CAP * n_y
    used = flight * SLOTS
    packed = cols + cols // 2
    hbm = pl.BlockSpec(memory_space=pltpu.HBM)

    def vmem(*shape, kind=BF):
        return pltpu.VMEM(shape, kind)

    dma = pltpu.SemaphoreType.DMA
    made = pl.pallas_call(
        functools.partial(kernel, n_s, n_e, n_d, steps),
        out_shape=(
            jax.ShapeDtypeStruct((1, steps, tok_rows, width), BF),
            jax.ShapeDtypeStruct((1, units, cols), F32),
        ),
        in_specs=[hbm] * 9,
        out_specs=(hbm, hbm),
        scratch_shapes=[
            vmem(CORES, n_d, units, cols),
            vmem(CORES, n_d, units, cols),
            vmem(CORES, n_d, units, cols),
            vmem(1, routes.shape[3], steps, tok_rows, kind=jnp.int32),
            vmem(1, routes.shape[3], steps, tok_rows),
            vmem(n_d, 1, cols, kind=F32),
            vmem(*cotangent.shape),
            vmem(n_d, tok_rows, cols),
            vmem(steps, n_d, tok_rows, cols),
            vmem(n_d, tok_rows, cols),
            vmem(steps, n_d, flight, 8, packed),
            vmem(steps, n_d, n_y, 8, packed),
            vmem(steps, n_d, flight, 8, packed),
            vmem(steps, n_d, n_y, 8, packed),
            vmem(steps, CORES, n_d, n_y, 8, packed),
            vmem(n_d, rows, cols),
            vmem(2, CORES, rows, units, kind=F32),
            vmem(steps, CORES, rows, units),
            vmem(steps, CORES * n_d, rows, units),
            vmem(2, CORES, 16 * n_y, units),
            vmem(steps, n_d, n_y, 8, packed),
            vmem(steps, n_d, n_y, 8, packed),
            vmem(used, tok_rows),
            vmem(used, tok_rows),
            vmem(n_d, tok_rows, cols),
            vmem(n_d, tok_rows, cols),
            vmem(units, cols, kind=F32),
            dma((6 + 3 * n_d,)),
            dma((n_d + 1,)),
            dma((3, 8)),
            dma((3, 8)),
            dma((SEMS,)),
            dma((SEMS,)),
        ],
        compiler_params=pltpu.CompilerParams(
            collective_id=0, has_side_effects=True, vmem_limit_bytes=60000 * 1024
        ),
    )(
        arrivals, fresh, jnp.transpose(routes, (0, 3, 1, 2)),
        jnp.transpose(gates, (0, 3, 1, 2)), cotangent,
        norm_gain, w_gate, w_up, w_down,
    )
    pieces = steps * 2 + 4
    return pl.pallas_call(
        finish,
        out_shape=tuple(jax.ShapeDtypeStruct(m.shape, m.dtype) for m in made),
        in_specs=[hbm] * 2,
        out_specs=(hbm, hbm),
        scratch_shapes=[pltpu.VMEM(m.shape, m.dtype) for m in made]
        + [pltpu.SemaphoreType.DMA((pieces,)), pltpu.SemaphoreType.DMA((pieces,))],
        compiler_params=pltpu.CompilerParams(vmem_limit_bytes=60000 * 1024),
    )(*made)


def solution(mesh):
    placed = (
        P("section", ("expert", "dp"), None),
        P(None, ("expert", "dp"), None),
        P("section", None, ("expert", "dp"), None),
        P("section", None, ("expert", "dp"), None),
        P("section", None, ("expert", "dp"), None),
        P("section", None),
        P("section", "expert", "dp"),
        P("section", "expert", "dp"),
        P("section", "expert", "dp"),
    )
    sizes = (mesh.shape["section"], mesh.shape["expert"], mesh.shape["dp"])
    return jax.shard_map(
        functools.partial(local, sizes),
        mesh=mesh,
        in_specs=placed,
        out_specs=(P("section", None, ("expert", "dp"), None), P("section", "expert", "dp")),
        check_vma=False,
    )
```

```python
import functools

import jax
import jax.numpy as jnp
from jax import lax
from jax.experimental import pallas as pl
from jax.experimental.pallas import tpu as pltpu
from jax.sharding import PartitionSpec as P

SPLIT = 4
CAP = 12
SLOTS = 16
CORES = 2
PAIRS = SPLIT // CORES
MESH = pl.DeviceIdType.MESH
BF = jnp.bfloat16
F32 = jnp.float32

TOK, COT, CROSS, SWAP, HID, RET, PICK, BASE, BACK, SEMS = 0, 8, 10, 12, 14, 16, 27, 28, 29, 30
NEAR, NEXT, RING, WRAP, CROSSED, TWIN, READY = 0, 4, 5, 6, 7, 8, 9


def mm(a, b, ca=1, cb=0):
    return lax.dot_general(a, b, (((ca,), (cb,)), ((), ())), preferred_element_type=F32)


def kernel(
    n_s, n_e, n_d, steps,
    arr_h, fresh_h, routes_h, gates_h, cot_h, gain_h, wg_h, wu_h, wd_h,
    out, grad,
    wg, wu, wd, routes, gates, gain, cot, fresh, inc, base,
    toks, tokr, cots, cotr, cotx, xg, acc, hid_s, hidr, hp, rets, retr,
    pick_s, pick_r, back, out_v, grad_v,
    load_sems, store_sems, w_send, w_recv, d_send, d_recv, send_sems, recv_sems, ready,
):
    sec = lax.axis_index("section")
    exp = lax.axis_index("expert")
    dp = lax.axis_index("dp")
    n_y = n_e // CORES
    flight = n_e // SPLIT
    n_c, rows, cols = inc.shape[1:]
    half = cols // 2
    units = wd.shape[3]
    part_units = units // 2
    width = cols * n_c
    used = flight * SLOTS
    n_low = 8 * n_y
    core = lax.rem(exp, CORES)
    y = exp // CORES
    sibling = (sec, exp + 1 - 2 * core, dp)
    nxt = lax.rem(sec + 1, n_s)
    prv = lax.rem(sec + n_s - 1, n_s)
    right = lax.rem(dp + 1, n_d)
    left = lax.rem(dp + n_d - 1, n_d)
    opp = lax.rem(dp + 2, n_d)
    to_right = (sec, exp, right)
    to_left = (sec, exp, left)
    to_next = (nxt, exp, dp)
    to_prev = (prv, exp, dp)
    offs = sorted(range(1, n_y), key=lambda o: -min(o, n_y - o))
    last = steps - 1

    def row(o):
        return lax.rem(y + o, n_y)

    above = (sec, row(1) * CORES + core, dp)
    below = (sec, row(n_y - 1) * CORES + core, dp)
    first_sec = sec == 0
    last_sec = sec == n_s - 1

    barrier = pltpu.get_barrier_semaphore()

    def signal(target):
        pl.semaphore_signal(barrier, inc=1, device_id=target, device_id_type=MESH)

    for target in (to_right, to_left, sibling, above, below):
        signal(target)

    @pl.when(jnp.logical_not(last_sec))
    def _():
        signal(to_next)

    @pl.when(first_sec)
    def _():
        signal(to_prev)

    greeted = 5 + jnp.minimum(sec, 1) + sec // (n_s - 1)

    def tell(i, *targets):
        for target in targets:
            pl.semaphore_signal(ready.at[i], inc=1, device_id=target, device_id_type=MESH)

    def told(i, n):
        pl.semaphore_wait(ready.at[i], n)

    def ring(i):
        told(NEAR + i, 2)
        if i < 3:
            tell(NEAR + i + 1, above, below)

    loads = []

    def load(src, dst):
        copy = pltpu.make_async_copy(src, dst, load_sems.at[len(loads)])
        copy.start()
        loads.append(copy)
        return copy

    def piece(c):
        return pl.ds(c * cols, cols)

    subs = range(n_c)
    load_w = [load(wg_h.at[0], wg.at[core, dp]), load(wu_h.at[0], wu.at[core, dp])]
    load_r = [load(routes_h, routes), load(gates_h, gates)]
    load_a = [load(arr_h.at[0, :, piece(c)], inc.at[0, c]) for c in subs]
    load_d = [load(wd_h.at[0, :, piece(q)], wd.at[core, dp, q]) for q in range(2)]
    load_c = load(cot_h, cot)
    load_g = [load(gain_h.at[:, piece(c)], gain.at[c]) for c in subs]
    load_f = [load(fresh_h.at[0, :, piece(c)], fresh.at[c]) for c in subs]

    def remote(src, dst, sem, target):
        return pltpu.make_async_remote_copy(
            src_ref=src, dst_ref=dst, send_sem=send_sems.at[sem], recv_sem=recv_sems.at[sem],
            device_id=target, device_id_type=MESH,
        )

    def got(ref, sem):
        remote(ref, ref, sem, sibling).wait_recv()

    def sent(ref, sem):
        remote(ref, ref, sem, sibling).wait_send()

    mats = (wg, wu)

    def w_copy(ref, m, i, target):
        return pltpu.make_async_remote_copy(
            src_ref=ref, dst_ref=ref, send_sem=w_send.at[m, i], recv_sem=w_recv.at[m, i],
            device_id=target, device_id_type=MESH,
        )

    def w_own(m):
        load_w[m].wait()
        mine = mats[m].at[core, dp]
        w_copy(mine, m, 0, to_right).start()
        w_copy(mine, m, 1, to_left).start()
        w_copy(mine, m, 4, sibling).start()

    def w_pass(m):
        w = mats[m]
        w_copy(w.at[core, left], m, 0, sibling).wait_recv()
        w_copy(w.at[core, left, pl.ds(0, part_units)], m, 2, to_right).start()
        w_copy(w.at[core, left], m, 5, sibling).start()
        w_copy(w.at[core, right], m, 1, sibling).wait_recv()
        w_copy(w.at[core, right, pl.ds(part_units, part_units)], m, 3, to_left).start()
        w_copy(w.at[core, right], m, 6, sibling).start()

    def w_last(m):
        for h in range(2):
            ref = mats[m].at[core, opp, pl.ds(h * part_units, part_units)]
            w_copy(ref, m, 2 + h, sibling).wait_recv()
            w_copy(ref, m, 7 + h, sibling).start()

    def w_twin(m, i):
        if i < 3:
            w_copy(mats[m].at[1 - core, (dp, left, right)[i]], m, 4 + i, sibling).wait_recv()
        else:
            for h in range(2):
                ref = mats[m].at[1 - core, opp, pl.ds(h * part_units, part_units)]
                w_copy(ref, m, 7 + h, sibling).wait_recv()

    def d_copy(ref, i, target):
        return pltpu.make_async_remote_copy(
            src_ref=ref, dst_ref=ref, send_sem=d_send.at[i], recv_sem=d_recv.at[i],
            device_id=target, device_id_type=MESH,
        )

    def d_own():
        for q in range(2):
            load_d[q].wait()
            d_copy(wd.at[core, dp, q], q, to_right).start()
            d_copy(wd.at[core, dp, q], 2 + q, to_left).start()
        d_copy(wd.at[core, dp], 8, sibling).start()

    def d_pass(q):
        d_copy(wd.at[core, left, q], q, sibling).wait_recv()
        d_copy(wd.at[core, left, q, pl.ds(0, part_units)], 4 + q, to_right).start()
        d_copy(wd.at[core, left, q], 10 + q, sibling).start()
        d_copy(wd.at[core, right, q], 2 + q, sibling).wait_recv()
        d_copy(wd.at[core, right, q, pl.ds(part_units, part_units)], 6 + q, to_left).start()
        d_copy(wd.at[core, right, q], 12 + q, sibling).start()

    def d_last(q):
        for h in range(2):
            ref = wd.at[core, opp, q, pl.ds(h * part_units, part_units)]
            d_copy(ref, 4 + 2 * h + q, sibling).wait_recv()
            d_copy(ref, 14 + 2 * q + h, sibling).start()

    def d_twin(name, q):
        if name == "own":
            d_copy(wd.at[1 - core, dp], 8, sibling).wait_recv()
        elif name == "left":
            d_copy(wd.at[1 - core, left, q], 10 + q, sibling).wait_recv()
        elif name == "right":
            d_copy(wd.at[1 - core, right, q], 12 + q, sibling).wait_recv()
        else:
            for h in range(2):
                ref = wd.at[1 - core, opp, q, pl.ds(h * part_units, part_units)]
                d_copy(ref, 14 + 2 * q + h, sibling).wait_recv()

    lane = lax.broadcasted_iota(jnp.int32, (used, rows), 0)
    lane_expert = lane >> 4
    lane_slot = lane & (SLOTS - 1)
    t_row = lax.broadcasted_iota(jnp.int32, (rows, rows), 0)
    t_col = lax.broadcasted_iota(jnp.int32, (rows, rows), 1)
    earlier_tok = jnp.where(t_row < t_col, 1.0, 0.0).astype(BF)

    def selection(k):
        naming = jnp.zeros((used, rows), F32)
        shares = jnp.zeros((used, rows), F32)
        for j in range(routes.shape[1]):
            hit = routes[0, j, k:k + 1, :] == lane_expert
            naming = jnp.where(hit, 1.0, naming)
            shares = shares + jnp.where(hit, gates[0, j].astype(F32)[k:k + 1, :], 0.0)
        places = mm(naming.astype(BF), earlier_tok)
        chosen = jnp.where(places == lane_slot.astype(F32), naming, 0.0)
        chosen = jnp.where(lane_slot < CAP, chosen, 0.0)
        return chosen.astype(BF), (chosen * shares).astype(BF)

    r_i = lax.broadcasted_iota(jnp.int32, (CAP * n_y, n_low), 0)
    c_i = lax.broadcasted_iota(jnp.int32, (CAP * n_y, n_low), 1)
    c_slot = c_i & 7
    shift = r_i - (c_i >> 3) * CAP - c_slot
    low_rows = jnp.where(shift == 0, 1.0, 0.0)
    tail_a = jnp.where((shift == 8) & (c_slot < 4), 1.0, 0.0)
    tail_b = jnp.where((shift == 4) & (c_slot >= 4), 1.0, 0.0)
    layout = jnp.concatenate([low_rows, tail_a, tail_b], axis=1).astype(BF)
    blank = jnp.zeros((n_low, half), BF)

    def swap(block):
        return jnp.concatenate([block[4:], block[:4]], axis=0)

    def fill(store, k, c, block):
        for f in range(flight):
            top = block[f * SLOTS:f * SLOTS + 8]
            bottom = block[f * SLOTS + 8:(f + 1) * SLOTS]
            store[k, c, f, :, :cols] = top.astype(BF)
            store[k, c, f, :, cols:] = (bottom[:, :half] + swap(bottom[:, half:])).astype(BF)

    def unpack(landing, *at):
        flat = landing[at].reshape(n_low, cols + half)
        tail = flat[:, cols:]
        stacked = jnp.concatenate(
            [
                flat[:, :cols],
                jnp.concatenate([tail, blank], axis=1),
                jnp.concatenate([blank, tail], axis=1),
            ],
            axis=0,
        )
        return mm(layout, stacked)

    def spread_all(store, landing, k, sem):
        for o in offs:
            remote(
                store.at[k, pl.ds(0, n_c), row(o) // PAIRS],
                landing.at[k, pl.ds(0, n_c), y], sem, (sec, row(o) * CORES + core, dp),
            ).start()
        for c in subs:
            landing[k, c, y] = store[k, c, y // PAIRS]

    def spread_some(store, landing, k, sub, n, sem):
        for o in offs:
            remote(
                store.at[k, pl.ds(sub, n), row(o) // PAIRS], landing.at[k, pl.ds(sub, n), y],
                sem, (sec, row(o) * CORES + core, dp),
            ).start()
        for q in range(n):
            landing[k, sub + q, y] = store[k, sub + q, y // PAIRS]

    def prepare(k, c):
        block = unpack(tokr, k, c)
        xg[c] = (block * gain[c]).astype(BF)
        return jnp.sum(block * block, axis=1, keepdims=True)

    def contract(parts, first, cores):
        for c in cores:
            for i, w in enumerate(mats):
                total = sum(
                    mm(xg[2 * ch + q], w[c, ch, :, q * cols:(q + 1) * cols], 1, 1)
                    for ch, q in parts
                )
                acc[i, c] = total if first else acc[i, c] + total

    def send_hidden(k):
        slot = hidr.at[k, core * n_d + dp]
        for x in (opp, right, left):
            for c in range(CORES):
                there = y * CORES + c
                remote(hid_s.at[k, c], slot, HID + k, (sec, there, x)).start()
        remote(hid_s.at[k, 1 - core], slot, HID + k, sibling).start()
        hidr[k, core * n_d + dp] = hid_s[k, core]

    def activate(k, squares, early):
        scale = lax.rsqrt(squares * (1.0 / width) + 0.5)
        for c in range(CORES):
            act_g = acc[0, c] * scale
            hid_s[k, c] = (act_g / (1.0 + jnp.exp(-act_g)) * (acc[1, c] * scale)).astype(BF)
        if early:
            send_hidden(k)
        for c in range(CORES):
            hp[c] = mm(layout, hid_s[k, c], 0, 0).astype(BF)

    def down(k, ch, qs, i, late=None):
        sub = 2 * ch + qs[0]
        for q in qs:
            rows_out = mm(hp[core], wd[core, ch, q])
            if late is not None and q == qs[0]:
                d_twin(late, q)
            rows_out = rows_out + mm(hp[1 - core], wd[1 - core, ch, q])
            tail = rows_out[n_low:2 * n_low, :half] + rows_out[2 * n_low:, half:]
            rets[k, 2 * ch + q, :, :, :cols] = rows_out[:n_low].astype(BF).reshape(n_y, 8, cols)
            rets[k, 2 * ch + q, :, :, cols:] = tail.astype(BF).reshape(n_y, 8, half)
        there = sec if k == last else nxt
        span = pl.ds(sub, len(qs))
        for o in offs + ([] if k == last else [0]):
            remote(
                rets.at[k, span, row(o)], retr.at[k, span, y], RET + 7 * k + i,
                (there, row(o) * CORES + core, dp),
            ).start()
        if k == last:
            for q in qs:
                retr[k, 2 * ch + q, y] = rets[k, 2 * ch + q, y]

    row_8 = lax.broadcasted_iota(jnp.int32, (8, half), 0)

    def landed(k, ch, qs, i):
        n = n_y - 1 if k == last else n_y
        got(retr.at[k, pl.ds(2 * ch + qs[0], len(qs)), pl.ds(0, n)], RET + 7 * k + i)

    def combine(k, c, weights, inputs):
        tops = []
        for f in range(flight):
            total = sum(retr[k, c, f * PAIRS + p].astype(F32) for p in range(PAIRS))
            tail = total[:, cols:]
            tops.append(total[:, :cols])
            tops.append(jnp.concatenate(
                [jnp.where(row_8 < 4, tail, 0.0), jnp.where(row_8 < 4, swap(tail), 0.0)], axis=1
            ))
        mixed = jnp.concatenate(tops, axis=0)
        high = mixed.astype(BF)
        low = (mixed - high.astype(F32)).astype(BF)
        mixture = mm(weights, high, 0, 0) + mm(weights, low, 0, 0)
        return (inputs.astype(F32) + mixture).astype(BF)

    def at_cols(c):
        return pl.ds(pl.multiple_of(c * cols, cols), cols)

    pl.semaphore_wait(barrier, greeted)
    w_own(0)
    w_own(1)
    tell(NEAR, above, below)
    tell(CROSSED, to_right, to_left)

    @pl.when(jnp.logical_not(first_sec))
    def _():
        tell(NEXT, to_prev)

    @pl.when(last_sec)
    def _():
        tell(WRAP, to_next)

    for copy in load_r:
        copy.wait()
    picks = [selection(0)]
    pick_s[...] = picks[0][1]
    for copy in load_a:
        copy.wait()
    ring(0)
    told(CROSSED, 2)
    tell(TWIN, sibling)
    for c in subs:
        fill(toks, 0, c, mm(picks[0][0], inc[0, c]))
    ring(1)
    picks.append(selection(1))
    load_c.wait()
    for c in subs:
        fill(cots, 0, c, mm(picks[0][1], cot[0, 0, :, c * cols:(c + 1) * cols]))
    ring(2)

    @pl.when(jnp.logical_not(first_sec))
    def _():
        tell(RING, to_prev)

    spread_all(toks, tokr, 0, TOK)
    spread_all(cots, cotr, 0, COT)
    for c in subs:
        fill(cots, 1, c, mm(picks[1][1], cot[0, 1, :, c * cols:(c + 1) * cols]))
    spread_all(cots, cotr, 1, COT + 1)

    @pl.when(jnp.logical_not(last_sec))
    def _():
        told(NEXT, 1)

    remote(inc.at[0], base, BASE, to_next).start()
    remote(pick_s, pick_r, PICK, to_next).start()
    for copy in load_g + load_f:
        copy.wait()
    told(TWIN, 1)

    items = (
        (dp, (0, 1)), (right, (0,)), (left, (0,)), (right, (1,)), (left, (1,)),
        (opp, (0,)), (opp, (1,)),
    )

    def enter(i, blocks):
        ch, qs = items[i]
        for q, block in zip(qs, blocks):
            inc[1, 2 * ch + q] = block
            fill(toks, 1, 2 * ch + q, mm(picks[1][0], block))
        spread_some(toks, tokr, 1, 2 * ch + qs[0], len(qs), TOK + 1 + i)

    def settle(i):
        ch, qs = items[i]
        landed(0, ch, qs, i)
        results = []
        for q in qs:
            c = 2 * ch + q
            results.append(combine(0, c, pick_r[...], base[c]))
            back[c] = results[-1]
            remote(back.at[c], out.at[0, 0, :, at_cols(c)], BACK, to_prev).start()
        return results

    def relay(i):
        ch, qs = items[i]

        @pl.when(first_sec)
        def _():
            enter(i, [fresh[2 * ch + q] for q in qs])

        @pl.when(jnp.logical_not(first_sec))
        def _():
            enter(i, settle(i))

    def tok_in(i):
        ch, qs = items[i]
        got(tokr.at[1, pl.ds(2 * ch + qs[0], len(qs)), pl.ds(0, n_y - 1)], TOK + 1 + i)
        return sum(prepare(1, 2 * ch + q) for q in qs)

    def parts_of(*which):
        return [(items[i][0], q) for i in which for q in items[i][1]]

    near = parts_of(0, 1, 2, 3, 4)
    far = parts_of(5, 6)
    w_pass(0)
    got(tokr.at[0, pl.ds(0, n_c), pl.ds(0, n_y - 1)], TOK)
    squares = sum(prepare(0, c) for c in subs)
    w_pass(1)
    d_own()
    contract(near, True, (core,))
    for m in range(2):
        for i in range(3):
            w_twin(m, i)
    contract(near, True, (1 - core,))
    w_last(0)
    w_last(1)
    contract(far, False, (core,))
    w_twin(0, 3)
    w_twin(1, 3)
    contract(far, False, (1 - core,))
    activate(0, squares, False)
    ring(3)

    @pl.when(jnp.logical_not(last_sec))
    def _():
        told(RING, 1)

    down(0, dp, (0, 1), 0, "own")
    for q in range(2):
        d_pass(q)
        d_twin("right", q)
        down(0, right, (q,), 1 + 2 * q)
        d_twin("left", q)
        down(0, left, (q,), 2 + 2 * q)
    got(base, BASE)
    got(pick_r, PICK)
    d_last(0)
    down(0, opp, (0,), 5, "opp")
    relay(0)
    d_last(1)
    down(0, opp, (1,), 6, "opp")
    send_hidden(0)
    for k in range(steps):
        got(cotr.at[k, pl.ds(0, n_c), pl.ds(0, n_y - 1)], COT + k)
        for x in (opp, right, left):
            remote(
                cotr.at[k, pl.ds(2 * x, 2)], cotx.at[k, core, dp], CROSS + k, (sec, exp, x)
            ).start()
        for q in range(2):
            cotx[k, core, dp, q] = cotr[k, 2 * dp + q]
    relay(1)
    relay(2)
    relay(3)
    relay(4)
    squares = tok_in(0)
    relay(5)
    relay(6)
    squares = squares + tok_in(1) + tok_in(2)
    contract(parts_of(0, 1, 2), True, (0, 1))
    squares = squares + tok_in(3) + tok_in(4)
    squares = squares + tok_in(5)
    contract(parts_of(3, 4, 5), False, (0, 1))
    squares = squares + tok_in(6)
    contract(parts_of(6), False, (0, 1))
    activate(1, squares, True)
    order = (dp, right, left, opp)
    for i, ch in enumerate(order):
        down(1, ch, (0, 1), i)

    @pl.when(first_sec)
    def _():
        told(WRAP, 1)
        for i in range(len(items)):
            settle(i)

    for k in range(steps):
        got(cotx.at[k, core, pl.ds(0, n_d - 1)], CROSS + k)
        remote(cotx.at[k, core], cotx.at[k, core], SWAP + k, sibling).start()
    for k in range(steps):
        got(cotx.at[k, 0], SWAP + k)
        got(hidr.at[k, pl.ds(0, CORES * n_d - 1)], HID + k)
        total = 0.0
        for c in range(CORES):
            rows_cot = jnp.concatenate(
                [
                    jnp.concatenate(
                        [unpack(cotx, k, c, x, q).astype(BF) for q in range(2)], axis=1
                    )
                    for x in range(n_d)
                ],
                axis=0,
            )
            rows_hid = hidr[k, pl.ds(c * n_d, n_d)].reshape(n_d * CAP * n_y, units)
            total = total + mm(rows_hid, rows_cot, 0, 0)
        grad_v[...] = total if k == 0 else grad_v[...] + total
    save_g = pltpu.make_async_copy(grad_v, grad.at[0], store_sems.at[n_c])
    save_g.start()
    saves = [save_g]
    for i, ch in enumerate(order):
        landed(1, ch, (0, 1), i)
        for q in range(2):
            c = 2 * ch + q
            out_v[c] = combine(1, c, picks[1][1], inc[1, c])
            save = pltpu.make_async_copy(
                out_v.at[c], out.at[0, 1, :, at_cols(c)], store_sems.at[2 * i + q]
            )
            save.start()
            saves.append(save)

    got(back, BACK)
    for m in range(2):
        w = mats[m]
        for i in (0, 1, 4, 5, 6):
            w_copy(w.at[0, 0], m, i, sibling).wait_send()
        for i in (2, 3, 7, 8):
            w_copy(w.at[0, 0, pl.ds(0, part_units)], m, i, sibling).wait_send()
    for i in (0, 1, 2, 3, 10, 11, 12, 13):
        d_copy(wd.at[0, 0, 0], i, sibling).wait_send()
    for i in (4, 5, 6, 7, 14, 15, 16, 17):
        d_copy(wd.at[0, 0, 0, pl.ds(0, part_units)], i, sibling).wait_send()
    d_copy(wd.at[0, 0], 8, sibling).wait_send()
    sent(tokr.at[0, pl.ds(0, n_c), pl.ds(0, n_y - 1)], TOK)
    for i, (ch, qs) in enumerate(items):
        sent(tokr.at[1, pl.ds(0, len(qs)), pl.ds(0, n_y - 1)], TOK + 1 + i)
        sent(rets.at[0, pl.ds(0, len(qs))], RET + i)
    for i in range(n_d):
        sent(rets.at[1, pl.ds(0, 2), pl.ds(0, n_y - 1)], RET + 7 + i)
    for k in range(steps):
        sent(cotr.at[k, pl.ds(0, n_c), pl.ds(0, n_y - 1)], COT + k)
        sent(cotx.at[k, 0, pl.ds(0, n_d - 1)], CROSS + k)
        sent(cotx.at[k, 0], SWAP + k)
        sent(hidr.at[k, pl.ds(0, CORES * n_d - 1)], HID + k)
    sent(pick_s, PICK)
    sent(base, BASE)
    sent(back, BACK)
    for save in saves:
        save.wait()


def finish(out_in, grad_in, out, grad, out_v, grad_v, in_sems, out_sems):
    steps, tok_rows = out_v.shape[1:3]
    units = grad_v.shape[1]
    moves = []
    for k in range(steps):
        for h in range(2):
            part = (0, k, pl.ds(h * tok_rows // 2, tok_rows // 2))
            moves.append((out_in.at[part], out_v.at[part], out.at[part]))
    for h in range(4):
        part = (0, pl.ds(h * units // 4, units // 4))
        moves.append((grad_in.at[part], grad_v.at[part], grad.at[part]))
    loads = [
        pltpu.make_async_copy(src, held, in_sems.at[i]) for i, (src, held, _) in enumerate(moves)
    ]
    stores = [
        pltpu.make_async_copy(held, dst, out_sems.at[i]) for i, (_, held, dst) in enumerate(moves)
    ]
    for load in loads:
        load.start()
    for load, store in zip(loads, stores):
        load.wait()
        store.start()
    for store in stores:
        store.wait()


def local(sizes, arrivals, fresh, routes, gates, cotangent, norm_gain, w_gate, w_up, w_down):
    n_s, n_e, n_d = sizes
    steps = routes.shape[1]
    tok_rows, width = arrivals.shape[1:]
    units, cols = w_gate.shape[1:]
    flight = n_e // SPLIT
    n_y = n_e // CORES
    n_c = 2 * n_d
    rows = CAP * n_y
    used = flight * SLOTS
    sub = cols // 2
    packed = sub + sub // 2
    hbm = pl.BlockSpec(memory_space=pltpu.HBM)

    def vmem(*shape, kind=BF):
        return pltpu.VMEM(shape, kind)

    dma = pltpu.SemaphoreType.DMA
    made = pl.pallas_call(
        functools.partial(kernel, n_s, n_e, n_d, steps),
        out_shape=(
            jax.ShapeDtypeStruct((1, steps, tok_rows, width), BF),
            jax.ShapeDtypeStruct((1, units, cols), F32),
        ),
        in_specs=[hbm] * 9,
        out_specs=(hbm, hbm),
        scratch_shapes=[
            vmem(CORES, n_d, units, cols),
            vmem(CORES, n_d, units, cols),
            vmem(CORES, n_d, 2, units, sub),
            vmem(1, routes.shape[3], steps, tok_rows, kind=jnp.int32),
            vmem(1, routes.shape[3], steps, tok_rows),
            vmem(n_c, 1, sub, kind=F32),
            vmem(*cotangent.shape),
            vmem(n_c, tok_rows, sub),
            vmem(steps, n_c, tok_rows, sub),
            vmem(n_c, tok_rows, sub),
            vmem(steps, n_c, flight, 8, packed),
            vmem(steps, n_c, n_y, 8, packed),
            vmem(steps, n_c, flight, 8, packed),
            vmem(steps, n_c, n_y, 8, packed),
            vmem(steps, CORES, n_d, 2, n_y, 8, packed),
            vmem(n_c, rows, sub),
            vmem(2, CORES, rows, units, kind=F32),
            vmem(steps, CORES, rows, units),
            vmem(steps, CORES * n_d, rows, units),
            vmem(CORES, 24 * n_y, units),
            vmem(steps, n_c, n_y, 8, packed),
            vmem(steps, n_c, n_y, 8, packed),
            vmem(used, tok_rows),
            vmem(used, tok_rows),
            vmem(n_c, tok_rows, sub),
            vmem(n_c, tok_rows, sub),
            vmem(units, cols, kind=F32),
            dma((7 + 3 * n_c,)),
            dma((n_c + 1,)),
            dma((2, 9)),
            dma((2, 9)),
            dma((18,)),
            dma((18,)),
            dma((SEMS,)),
            dma((SEMS,)),
            pltpu.SemaphoreType.REGULAR((READY,)),
        ],
        compiler_params=pltpu.CompilerParams(
            collective_id=0, has_side_effects=True, vmem_limit_bytes=60000 * 1024
        ),
    )(
        arrivals, fresh, jnp.transpose(routes, (0, 3, 1, 2)),
        jnp.transpose(gates, (0, 3, 1, 2)), cotangent,
        norm_gain, w_gate, w_up, w_down,
    )
    pieces = steps * 2 + 4
    return pl.pallas_call(
        finish,
        out_shape=tuple(jax.ShapeDtypeStruct(m.shape, m.dtype) for m in made),
        in_specs=[hbm] * 2,
        out_specs=(hbm, hbm),
        scratch_shapes=[pltpu.VMEM(m.shape, m.dtype) for m in made]
        + [pltpu.SemaphoreType.DMA((pieces,)), pltpu.SemaphoreType.DMA((pieces,))],
        compiler_params=pltpu.CompilerParams(vmem_limit_bytes=60000 * 1024),
    )(*made)


def solution(mesh):
    placed = (
        P("section", ("expert", "dp"), None),
        P(None, ("expert", "dp"), None),
        P("section", None, ("expert", "dp"), None),
        P("section", None, ("expert", "dp"), None),
        P("section", None, ("expert", "dp"), None),
        P("section", None),
        P("section", "expert", "dp"),
        P("section", "expert", "dp"),
        P("section", "expert", "dp"),
    )
    sizes = (mesh.shape["section"], mesh.shape["expert"], mesh.shape["dp"])
    return jax.shard_map(
        functools.partial(local, sizes),
        mesh=mesh,
        in_specs=placed,
        out_specs=(P("section", None, ("expert", "dp"), None), P("section", "expert", "dp")),
        check_vma=False,
    )
```

```python
import functools

import jax
import jax.numpy as jnp
from jax import lax
from jax.experimental import pallas as pl
from jax.experimental.pallas import tpu as pltpu
from jax.sharding import PartitionSpec as P

SPLIT = 4
CAP = 12
SLOTS = 16
CORES = 2
PAIRS = SPLIT // CORES
MESH = pl.DeviceIdType.MESH
BF = jnp.bfloat16
F32 = jnp.float32

TOK, COT, CROSS, SWAP, HID, RET, PICK, BASE, BACK, SEMS = 0, 8, 10, 12, 14, 16, 27, 28, 29, 30
NEAR, NEXT, RING, WRAP, CROSSED, TWIN, READY = 0, 4, 5, 6, 7, 8, 9


def mm(a, b, ca=1, cb=0):
    return lax.dot_general(a, b, (((ca,), (cb,)), ((), ())), preferred_element_type=F32)


def kernel(
    n_s, n_e, n_d, steps,
    arr_h, fresh_h, routes_h, gates_h, cot_h, gain_h, wg_h, wu_h, wd_h,
    out, grad,
    wg, wu, wd, routes, gates, gain, cot, fresh, inc, base,
    toks, tokr, cots, cotr, cotx, xg, acc, hid_s, hidr, hp, rets, retr,
    pick_s, pick_r, back,
    load_sems, w_send, w_recv, d_send, d_recv, send_sems, recv_sems, ready,
):
    sec = lax.axis_index("section")
    exp = lax.axis_index("expert")
    dp = lax.axis_index("dp")
    n_y = n_e // CORES
    flight = n_e // SPLIT
    n_c, rows, cols = inc.shape[1:]
    half = cols // 2
    units = wd.shape[3]
    part_units = units // 2
    width = cols * n_c
    used = flight * SLOTS
    n_low = 8 * n_y
    core = lax.rem(exp, CORES)
    y = exp // CORES
    sibling = (sec, exp + 1 - 2 * core, dp)
    nxt = lax.rem(sec + 1, n_s)
    prv = lax.rem(sec + n_s - 1, n_s)
    right = lax.rem(dp + 1, n_d)
    left = lax.rem(dp + n_d - 1, n_d)
    opp = lax.rem(dp + 2, n_d)
    to_right = (sec, exp, right)
    to_left = (sec, exp, left)
    to_next = (nxt, exp, dp)
    to_prev = (prv, exp, dp)
    offs = sorted(range(1, n_y), key=lambda o: -min(o, n_y - o))
    last = steps - 1

    def row(o):
        return lax.rem(y + o, n_y)

    above = (sec, row(1) * CORES + core, dp)
    below = (sec, row(n_y - 1) * CORES + core, dp)
    first_sec = sec == 0
    last_sec = sec == n_s - 1

    barrier = pltpu.get_barrier_semaphore()

    def signal(target):
        pl.semaphore_signal(barrier, inc=1, device_id=target, device_id_type=MESH)

    for target in (to_right, to_left, sibling, above, below):
        signal(target)

    @pl.when(jnp.logical_not(last_sec))
    def _():
        signal(to_next)

    @pl.when(first_sec)
    def _():
        signal(to_prev)

    greeted = 5 + jnp.minimum(sec, 1) + sec // (n_s - 1)

    def tell(i, *targets):
        for target in targets:
            pl.semaphore_signal(ready.at[i], inc=1, device_id=target, device_id_type=MESH)

    def told(i, n):
        pl.semaphore_wait(ready.at[i], n)

    def ring(i):
        told(NEAR + i, 2)
        if i < 3:
            tell(NEAR + i + 1, above, below)

    loads = []

    def load(src, dst):
        copy = pltpu.make_async_copy(src, dst, load_sems.at[len(loads)])
        copy.start()
        loads.append(copy)
        return copy

    def piece(c):
        return pl.ds(c * cols, cols)

    subs = range(n_c)
    load_w = [load(wg_h.at[0], wg.at[core, dp]), load(wu_h.at[0], wu.at[core, dp])]
    load_r = [load(routes_h, routes), load(gates_h, gates)]
    load_a = [load(arr_h.at[0, :, piece(c)], inc.at[0, c]) for c in subs]
    load_d = [load(wd_h.at[0, :, piece(q)], wd.at[core, dp, q]) for q in range(2)]
    load_c = load(cot_h, cot)
    load_g = [load(gain_h.at[:, piece(c)], gain.at[c]) for c in subs]
    load_f = [load(fresh_h.at[0, :, piece(c)], fresh.at[c]) for c in subs]

    def remote(src, dst, sem, target):
        return pltpu.make_async_remote_copy(
            src_ref=src, dst_ref=dst, send_sem=send_sems.at[sem], recv_sem=recv_sems.at[sem],
            device_id=target, device_id_type=MESH,
        )

    def got(ref, sem):
        remote(ref, ref, sem, sibling).wait_recv()

    def sent(ref, sem):
        remote(ref, ref, sem, sibling).wait_send()

    mats = (wg, wu)

    def w_copy(ref, m, i, target):
        return pltpu.make_async_remote_copy(
            src_ref=ref, dst_ref=ref, send_sem=w_send.at[m, i], recv_sem=w_recv.at[m, i],
            device_id=target, device_id_type=MESH,
        )

    def w_own(m):
        load_w[m].wait()
        mine = mats[m].at[core, dp]
        w_copy(mine, m, 0, to_right).start()
        w_copy(mine, m, 1, to_left).start()
        w_copy(mine, m, 4, sibling).start()

    def w_pass(m):
        w = mats[m]
        w_copy(w.at[core, left], m, 0, sibling).wait_recv()
        w_copy(w.at[core, left, pl.ds(0, part_units)], m, 2, to_right).start()
        w_copy(w.at[core, left], m, 5, sibling).start()
        w_copy(w.at[core, right], m, 1, sibling).wait_recv()
        w_copy(w.at[core, right, pl.ds(part_units, part_units)], m, 3, to_left).start()
        w_copy(w.at[core, right], m, 6, sibling).start()

    def w_last(m):
        for h in range(2):
            ref = mats[m].at[core, opp, pl.ds(h * part_units, part_units)]
            w_copy(ref, m, 2 + h, sibling).wait_recv()
            w_copy(ref, m, 7 + h, sibling).start()

    def w_twin(m, i):
        if i < 3:
            w_copy(mats[m].at[1 - core, (dp, left, right)[i]], m, 4 + i, sibling).wait_recv()
        else:
            for h in range(2):
                ref = mats[m].at[1 - core, opp, pl.ds(h * part_units, part_units)]
                w_copy(ref, m, 7 + h, sibling).wait_recv()

    def d_copy(ref, i, target):
        return pltpu.make_async_remote_copy(
            src_ref=ref, dst_ref=ref, send_sem=d_send.at[i], recv_sem=d_recv.at[i],
            device_id=target, device_id_type=MESH,
        )

    def d_own():
        for q in range(2):
            load_d[q].wait()
            d_copy(wd.at[core, dp, q], q, to_right).start()
            d_copy(wd.at[core, dp, q], 2 + q, to_left).start()
        d_copy(wd.at[core, dp], 8, sibling).start()

    def d_pass(q):
        d_copy(wd.at[core, left, q], q, sibling).wait_recv()
        d_copy(wd.at[core, left, q, pl.ds(0, part_units)], 4 + q, to_right).start()
        d_copy(wd.at[core, left, q], 10 + q, sibling).start()
        d_copy(wd.at[core, right, q], 2 + q, sibling).wait_recv()
        d_copy(wd.at[core, right, q, pl.ds(part_units, part_units)], 6 + q, to_left).start()
        d_copy(wd.at[core, right, q], 12 + q, sibling).start()

    def d_last(q):
        for h in range(2):
            ref = wd.at[core, opp, q, pl.ds(h * part_units, part_units)]
            d_copy(ref, 4 + 2 * h + q, sibling).wait_recv()
            d_copy(ref, 14 + 2 * q + h, sibling).start()

    def d_twin(name, q):
        if name == "own":
            d_copy(wd.at[1 - core, dp], 8, sibling).wait_recv()
        elif name == "left":
            d_copy(wd.at[1 - core, left, q], 10 + q, sibling).wait_recv()
        elif name == "right":
            d_copy(wd.at[1 - core, right, q], 12 + q, sibling).wait_recv()
        else:
            for h in range(2):
                ref = wd.at[1 - core, opp, q, pl.ds(h * part_units, part_units)]
                d_copy(ref, 14 + 2 * q + h, sibling).wait_recv()

    lane = lax.broadcasted_iota(jnp.int32, (used, rows), 0)
    lane_expert = lane >> 4
    lane_slot = lane & (SLOTS - 1)
    t_row = lax.broadcasted_iota(jnp.int32, (rows, rows), 0)
    t_col = lax.broadcasted_iota(jnp.int32, (rows, rows), 1)
    earlier_tok = jnp.where(t_row < t_col, 1.0, 0.0).astype(BF)

    def selection(k):
        naming = jnp.zeros((used, rows), F32)
        shares = jnp.zeros((used, rows), F32)
        for j in range(routes.shape[1]):
            hit = routes[0, j, k:k + 1, :] == lane_expert
            naming = jnp.where(hit, 1.0, naming)
            shares = shares + jnp.where(hit, gates[0, j].astype(F32)[k:k + 1, :], 0.0)
        places = mm(naming.astype(BF), earlier_tok)
        chosen = jnp.where(places == lane_slot.astype(F32), naming, 0.0)
        chosen = jnp.where(lane_slot < CAP, chosen, 0.0)
        return chosen.astype(BF), (chosen * shares).astype(BF)

    r_i = lax.broadcasted_iota(jnp.int32, (CAP * n_y, n_low), 0)
    c_i = lax.broadcasted_iota(jnp.int32, (CAP * n_y, n_low), 1)
    c_slot = c_i & 7
    shift = r_i - (c_i >> 3) * CAP - c_slot
    low_rows = jnp.where(shift == 0, 1.0, 0.0)
    tail_a = jnp.where((shift == 8) & (c_slot < 4), 1.0, 0.0)
    tail_b = jnp.where((shift == 4) & (c_slot >= 4), 1.0, 0.0)
    layout = jnp.concatenate([low_rows, tail_a, tail_b], axis=1).astype(BF)
    blank = jnp.zeros((n_low, half), BF)

    def swap(block):
        return jnp.concatenate([block[4:], block[:4]], axis=0)

    def fill(store, k, c, block):
        for f in range(flight):
            top = block[f * SLOTS:f * SLOTS + 8]
            bottom = block[f * SLOTS + 8:(f + 1) * SLOTS]
            store[k, c, f, :, :cols] = top.astype(BF)
            store[k, c, f, :, cols:] = (bottom[:, :half] + swap(bottom[:, half:])).astype(BF)

    def unpack(landing, *at):
        flat = landing[at].reshape(n_low, cols + half)
        tail = flat[:, cols:]
        stacked = jnp.concatenate(
            [
                flat[:, :cols],
                jnp.concatenate([tail, blank], axis=1),
                jnp.concatenate([blank, tail], axis=1),
            ],
            axis=0,
        )
        return mm(layout, stacked)

    def spread_all(store, landing, k, sem):
        for o in offs:
            remote(
                store.at[k, pl.ds(0, n_c), row(o) // PAIRS],
                landing.at[k, pl.ds(0, n_c), y], sem, (sec, row(o) * CORES + core, dp),
            ).start()
        for c in subs:
            landing[k, c, y] = store[k, c, y // PAIRS]

    def spread_some(store, landing, k, sub, n, sem):
        for o in offs:
            remote(
                store.at[k, pl.ds(sub, n), row(o) // PAIRS], landing.at[k, pl.ds(sub, n), y],
                sem, (sec, row(o) * CORES + core, dp),
            ).start()
        for q in range(n):
            landing[k, sub + q, y] = store[k, sub + q, y // PAIRS]

    def prepare(k, c):
        block = unpack(tokr, k, c)
        xg[c] = (block * gain[c]).astype(BF)
        return jnp.sum(block * block, axis=1, keepdims=True)

    def contract(parts, first, cores):
        for c in cores:
            for i, w in enumerate(mats):
                total = sum(
                    mm(xg[2 * ch + q], w[c, ch, :, q * cols:(q + 1) * cols], 1, 1)
                    for ch, q in parts
                )
                acc[i, c] = total if first else acc[i, c] + total

    def send_hidden(k):
        slot = hidr.at[k, core * n_d + dp]
        for x in (opp, right, left):
            for c in range(CORES):
                there = y * CORES + c
                remote(hid_s.at[k, c], slot, HID + k, (sec, there, x)).start()
        remote(hid_s.at[k, 1 - core], slot, HID + k, sibling).start()
        hidr[k, core * n_d + dp] = hid_s[k, core]

    def activate(k, squares, early):
        scale = lax.rsqrt(squares * (1.0 / width) + 0.5)
        for c in range(CORES):
            act_g = acc[0, c] * scale
            hid_s[k, c] = (act_g / (1.0 + jnp.exp(-act_g)) * (acc[1, c] * scale)).astype(BF)
        if early:
            send_hidden(k)
        for c in range(CORES):
            hp[c] = mm(layout, hid_s[k, c], 0, 0).astype(BF)

    def down(k, ch, qs, i, late=None):
        sub = 2 * ch + qs[0]
        for q in qs:
            rows_out = mm(hp[core], wd[core, ch, q])
            if late is not None and q == qs[0]:
                d_twin(late, q)
            rows_out = rows_out + mm(hp[1 - core], wd[1 - core, ch, q])
            tail = rows_out[n_low:2 * n_low, :half] + rows_out[2 * n_low:, half:]
            rets[k, 2 * ch + q, :, :, :cols] = rows_out[:n_low].astype(BF).reshape(n_y, 8, cols)
            rets[k, 2 * ch + q, :, :, cols:] = tail.astype(BF).reshape(n_y, 8, half)
        there = sec if k == last else nxt
        span = pl.ds(sub, len(qs))
        for o in offs + ([] if k == last else [0]):
            remote(
                rets.at[k, span, row(o)], retr.at[k, span, y], RET + 7 * k + i,
                (there, row(o) * CORES + core, dp),
            ).start()
        if k == last:
            for q in qs:
                retr[k, 2 * ch + q, y] = rets[k, 2 * ch + q, y]

    row_8 = lax.broadcasted_iota(jnp.int32, (8, half), 0)

    def landed(k, ch, qs, i):
        n = n_y - 1 if k == last else n_y
        got(retr.at[k, pl.ds(2 * ch + qs[0], len(qs)), pl.ds(0, n)], RET + 7 * k + i)

    def combine(k, c, weights, inputs):
        tops = []
        for f in range(flight):
            total = sum(retr[k, c, f * PAIRS + p].astype(F32) for p in range(PAIRS))
            tail = total[:, cols:]
            tops.append(total[:, :cols])
            tops.append(jnp.concatenate(
                [jnp.where(row_8 < 4, tail, 0.0), jnp.where(row_8 < 4, swap(tail), 0.0)], axis=1
            ))
        mixed = jnp.concatenate(tops, axis=0)
        high = mixed.astype(BF)
        low = (mixed - high.astype(F32)).astype(BF)
        mixture = mm(weights, high, 0, 0) + mm(weights, low, 0, 0)
        return (inputs.astype(F32) + mixture).astype(BF)

    def at_cols(c):
        return pl.ds(pl.multiple_of(c * cols, cols), cols)

    pl.semaphore_wait(barrier, greeted)
    w_own(0)
    w_own(1)
    tell(NEAR, above, below)
    tell(CROSSED, to_right, to_left)

    @pl.when(jnp.logical_not(first_sec))
    def _():
        tell(NEXT, to_prev)

    @pl.when(last_sec)
    def _():
        tell(WRAP, to_next)

    for copy in load_r:
        copy.wait()
    picks = [selection(0)]
    pick_s[...] = picks[0][1]
    for copy in load_a:
        copy.wait()
    ring(0)
    told(CROSSED, 2)
    tell(TWIN, sibling)
    for c in subs:
        fill(toks, 0, c, mm(picks[0][0], inc[0, c]))
    ring(1)
    picks.append(selection(1))
    load_c.wait()
    for c in subs:
        fill(cots, 0, c, mm(picks[0][1], cot[0, 0, :, c * cols:(c + 1) * cols]))
    ring(2)

    @pl.when(jnp.logical_not(first_sec))
    def _():
        tell(RING, to_prev)

    spread_all(toks, tokr, 0, TOK)
    spread_all(cots, cotr, 0, COT)
    for c in subs:
        fill(cots, 1, c, mm(picks[1][1], cot[0, 1, :, c * cols:(c + 1) * cols]))
    spread_all(cots, cotr, 1, COT + 1)

    @pl.when(jnp.logical_not(last_sec))
    def _():
        told(NEXT, 1)

    remote(inc.at[0], base, BASE, to_next).start()
    remote(pick_s, pick_r, PICK, to_next).start()
    for copy in load_g + load_f:
        copy.wait()
    told(TWIN, 1)

    items = (
        (dp, (0, 1)), (right, (0,)), (left, (0,)), (right, (1,)), (left, (1,)),
        (opp, (0,)), (opp, (1,)),
    )

    def enter(i, blocks):
        ch, qs = items[i]
        for q, block in zip(qs, blocks):
            inc[1, 2 * ch + q] = block
            fill(toks, 1, 2 * ch + q, mm(picks[1][0], block))
        spread_some(toks, tokr, 1, 2 * ch + qs[0], len(qs), TOK + 1 + i)

    def settle(i):
        ch, qs = items[i]
        landed(0, ch, qs, i)
        results = []
        for q in qs:
            c = 2 * ch + q
            results.append(combine(0, c, pick_r[...], base[c]))
            back[c] = results[-1]
            remote(back.at[c], out.at[0, 0, :, at_cols(c)], BACK, to_prev).start()
        return results

    def relay(i):
        ch, qs = items[i]

        @pl.when(first_sec)
        def _():
            enter(i, [fresh[2 * ch + q] for q in qs])

        @pl.when(jnp.logical_not(first_sec))
        def _():
            enter(i, settle(i))

    def tok_in(i):
        ch, qs = items[i]
        got(tokr.at[1, pl.ds(2 * ch + qs[0], len(qs)), pl.ds(0, n_y - 1)], TOK + 1 + i)
        return sum(prepare(1, 2 * ch + q) for q in qs)

    def parts_of(*which):
        return [(items[i][0], q) for i in which for q in items[i][1]]

    near = parts_of(0, 1, 2, 3, 4)
    far = parts_of(5, 6)
    w_pass(0)
    got(tokr.at[0, pl.ds(0, n_c), pl.ds(0, n_y - 1)], TOK)
    squares = sum(prepare(0, c) for c in subs)
    w_pass(1)
    d_own()
    contract(near, True, (core,))
    for m in range(2):
        for i in range(3):
            w_twin(m, i)
    contract(near, True, (1 - core,))
    w_last(0)
    w_last(1)
    contract(far, False, (core,))
    w_twin(0, 3)
    w_twin(1, 3)
    contract(far, False, (1 - core,))
    activate(0, squares, False)
    ring(3)

    @pl.when(jnp.logical_not(last_sec))
    def _():
        told(RING, 1)

    down(0, dp, (0, 1), 0, "own")
    d_pass(0)
    d_twin("right", 0)
    down(0, right, (0,), 1)
    d_twin("left", 0)
    down(0, left, (0,), 2)
    got(base, BASE)
    got(pick_r, PICK)
    d_pass(1)
    relay(0)
    d_twin("right", 1)
    down(0, right, (1,), 3)
    d_twin("left", 1)
    down(0, left, (1,), 4)
    d_last(0)
    send_hidden(0)
    for k in range(steps):
        got(cotr.at[k, pl.ds(0, n_c), pl.ds(0, n_y - 1)], COT + k)
        for x in (opp, right, left):
            remote(
                cotr.at[k, pl.ds(2 * x, 2)], cotx.at[k, core, dp], CROSS + k, (sec, exp, x)
            ).start()
        for q in range(2):
            cotx[k, core, dp, q] = cotr[k, 2 * dp + q]
    down(0, opp, (0,), 5, "opp")
    d_last(1)
    relay(1)
    down(0, opp, (1,), 6, "opp")
    relay(2)
    relay(3)
    relay(4)
    squares = tok_in(0)
    relay(5)
    relay(6)
    squares = squares + tok_in(1) + tok_in(2)
    contract(parts_of(0, 1, 2), True, (0, 1))
    squares = squares + tok_in(3) + tok_in(4)
    squares = squares + tok_in(5)
    contract(parts_of(3, 4, 5), False, (0, 1))
    squares = squares + tok_in(6)
    contract(parts_of(6), False, (0, 1))
    activate(1, squares, True)
    order = (dp, right, left, opp)
    for i, ch in enumerate(order):
        down(1, ch, (0, 1), i)

    @pl.when(first_sec)
    def _():
        told(WRAP, 1)
        for i in range(len(items)):
            settle(i)

    for k in range(steps):
        got(cotx.at[k, core, pl.ds(0, n_d - 1)], CROSS + k)
        remote(cotx.at[k, core], cotx.at[k, core], SWAP + k, sibling).start()
    for k in range(steps):
        got(cotx.at[k, 0], SWAP + k)
        got(hidr.at[k, pl.ds(0, CORES * n_d - 1)], HID + k)
        total = 0.0
        for c in range(CORES):
            rows_cot = jnp.concatenate(
                [
                    jnp.concatenate(
                        [unpack(cotx, k, c, x, q).astype(BF) for q in range(2)], axis=1
                    )
                    for x in range(n_d)
                ],
                axis=0,
            )
            rows_hid = hidr[k, pl.ds(c * n_d, n_d)].reshape(n_d * CAP * n_y, units)
            total = total + mm(rows_hid, rows_cot, 0, 0)
        grad[0] = total if k == 0 else grad[0] + total
    for i, ch in enumerate(order):
        landed(1, ch, (0, 1), i)
        for q in range(2):
            c = 2 * ch + q
            out[0, 1, :, at_cols(c)] = combine(1, c, picks[1][1], inc[1, c])

    got(back, BACK)
    for m in range(2):
        w = mats[m]
        for i in (0, 1, 4, 5, 6):
            w_copy(w.at[0, 0], m, i, sibling).wait_send()
        for i in (2, 3, 7, 8):
            w_copy(w.at[0, 0, pl.ds(0, part_units)], m, i, sibling).wait_send()
    for i in (0, 1, 2, 3, 10, 11, 12, 13):
        d_copy(wd.at[0, 0, 0], i, sibling).wait_send()
    for i in (4, 5, 6, 7, 14, 15, 16, 17):
        d_copy(wd.at[0, 0, 0, pl.ds(0, part_units)], i, sibling).wait_send()
    d_copy(wd.at[0, 0], 8, sibling).wait_send()
    sent(tokr.at[0, pl.ds(0, n_c), pl.ds(0, n_y - 1)], TOK)
    for i, (ch, qs) in enumerate(items):
        sent(tokr.at[1, pl.ds(0, len(qs)), pl.ds(0, n_y - 1)], TOK + 1 + i)
        sent(rets.at[0, pl.ds(0, len(qs))], RET + i)
    for i in range(n_d):
        sent(rets.at[1, pl.ds(0, 2), pl.ds(0, n_y - 1)], RET + 7 + i)
    for k in range(steps):
        sent(cotr.at[k, pl.ds(0, n_c), pl.ds(0, n_y - 1)], COT + k)
        sent(cotx.at[k, 0, pl.ds(0, n_d - 1)], CROSS + k)
        sent(cotx.at[k, 0], SWAP + k)
        sent(hidr.at[k, pl.ds(0, CORES * n_d - 1)], HID + k)
    sent(pick_s, PICK)
    sent(base, BASE)
    sent(back, BACK)


def finish(out_in, grad_in, out, grad, sems):
    pieces = ((out_in, out), (grad_in, grad))
    copies = [pltpu.make_async_copy(src, dst, sems.at[i]) for i, (src, dst) in enumerate(pieces)]
    for copy in copies:
        copy.start()
    for copy in copies:
        copy.wait()


def local(sizes, arrivals, fresh, routes, gates, cotangent, norm_gain, w_gate, w_up, w_down):
    n_s, n_e, n_d = sizes
    steps = routes.shape[1]
    tok_rows, width = arrivals.shape[1:]
    units, cols = w_gate.shape[1:]
    flight = n_e // SPLIT
    n_y = n_e // CORES
    n_c = 2 * n_d
    rows = CAP * n_y
    used = flight * SLOTS
    sub = cols // 2
    packed = sub + sub // 2
    hbm = pl.BlockSpec(memory_space=pltpu.HBM)
    held = pl.BlockSpec(memory_space=pltpu.VMEM)

    def vmem(*shape, kind=BF):
        return pltpu.VMEM(shape, kind)

    dma = pltpu.SemaphoreType.DMA
    made = pl.pallas_call(
        functools.partial(kernel, n_s, n_e, n_d, steps),
        out_shape=(
            pltpu.VMEM((1, steps, tok_rows, width), BF),
            pltpu.VMEM((1, units, cols), F32),
        ),
        in_specs=[hbm] * 9,
        out_specs=(held, held),
        scratch_shapes=[
            vmem(CORES, n_d, units, cols),
            vmem(CORES, n_d, units, cols),
            vmem(CORES, n_d, 2, units, sub),
            vmem(1, routes.shape[3], steps, tok_rows, kind=jnp.int32),
            vmem(1, routes.shape[3], steps, tok_rows),
            vmem(n_c, 1, sub, kind=F32),
            vmem(*cotangent.shape),
            vmem(n_c, tok_rows, sub),
            vmem(steps, n_c, tok_rows, sub),
            vmem(n_c, tok_rows, sub),
            vmem(steps, n_c, flight, 8, packed),
            vmem(steps, n_c, n_y, 8, packed),
            vmem(steps, n_c, flight, 8, packed),
            vmem(steps, n_c, n_y, 8, packed),
            vmem(steps, CORES, n_d, 2, n_y, 8, packed),
            vmem(n_c, rows, sub),
            vmem(2, CORES, rows, units, kind=F32),
            vmem(steps, CORES, rows, units),
            vmem(steps, CORES * n_d, rows, units),
            vmem(CORES, 24 * n_y, units),
            vmem(steps, n_c, n_y, 8, packed),
            vmem(steps, n_c, n_y, 8, packed),
            vmem(used, tok_rows),
            vmem(used, tok_rows),
            vmem(n_c, tok_rows, sub),
            dma((7 + 3 * n_c,)),
            dma((2, 9)),
            dma((2, 9)),
            dma((18,)),
            dma((18,)),
            dma((SEMS,)),
            dma((SEMS,)),
            pltpu.SemaphoreType.REGULAR((READY,)),
        ],
        compiler_params=pltpu.CompilerParams(
            collective_id=0, has_side_effects=True, vmem_limit_bytes=64240 * 1024
        ),
    )(
        arrivals, fresh, jnp.transpose(routes, (0, 3, 1, 2)),
        jnp.transpose(gates, (0, 3, 1, 2)), cotangent,
        norm_gain, w_gate, w_up, w_down,
    )
    return pl.pallas_call(
        finish,
        out_shape=tuple(jax.ShapeDtypeStruct(m.shape, m.dtype) for m in made),
        in_specs=[held] * 2,
        out_specs=(hbm, hbm),
        scratch_shapes=[pltpu.SemaphoreType.DMA((2,))],
        compiler_params=pltpu.CompilerParams(vmem_limit_bytes=4096 * 1024),
    )(*made)


def solution(mesh):
    placed = (
        P("section", ("expert", "dp"), None),
        P(None, ("expert", "dp"), None),
        P("section", None, ("expert", "dp"), None),
        P("section", None, ("expert", "dp"), None),
        P("section", None, ("expert", "dp"), None),
        P("section", None),
        P("section", "expert", "dp"),
        P("section", "expert", "dp"),
        P("section", "expert", "dp"),
    )
    sizes = (mesh.shape["section"], mesh.shape["expert"], mesh.shape["dp"])
    return jax.shard_map(
        functools.partial(local, sizes),
        mesh=mesh,
        in_specs=placed,
        out_specs=(P("section", None, ("expert", "dp"), None), P("section", "expert", "dp")),
        check_vma=False,
    )
```

```python
import functools

import jax
import jax.numpy as jnp
from jax import lax
from jax.experimental import pallas as pl
from jax.experimental.pallas import tpu as pltpu
from jax.sharding import PartitionSpec as P

SPLIT = 4
CAP = 12
SLOTS = 16
CORES = 2
PAIRS = SPLIT // CORES
MESH = pl.DeviceIdType.MESH
BF = jnp.bfloat16
F32 = jnp.float32

TOK, COT, CROSS, SWAP, HID, RET, PICK, BASE, BACK, PART, OVER, SEMS = 0, 8, 10, 12, 14, 16, 27, 28, 29, 30, 34, 35
SENDS = 10
NEAR, NEXT, RING, WRAP, CROSSED, TWIN, READY = 0, 4, 5, 6, 7, 8, 9


def mm(a, b, ca=1, cb=0):
    return lax.dot_general(a, b, (((ca,), (cb,)), ((), ())), preferred_element_type=F32)


def kernel(
    n_s, n_e, n_d, steps,
    arr_h, fresh_h, routes_h, gates_h, cot_h, gain_h, wg_h, wu_h, wd_h,
    out, grad,
    wg, wu, wd, routes, gates, gain, cot, fresh, inc, base,
    toks, tokr, cots, cotr, cotx, xg, acc, hid_s, hidr, hp, rets, retr,
    pick_s, pick_r, back,
    load_sems, w_send, w_recv, d_recv, send_sems, recv_sems, ready,
):
    sec = lax.axis_index("section")
    exp = lax.axis_index("expert")
    dp = lax.axis_index("dp")
    n_y = n_e // CORES
    flight = n_e // SPLIT
    n_c, rows, cols = back.shape
    half = cols // 2
    units = wd.shape[2]
    part_units = units // 2
    width = cols * n_c
    used = flight * SLOTS
    n_low = 8 * n_y
    core = lax.rem(exp, CORES)
    y = exp // CORES
    sibling = (sec, exp + 1 - 2 * core, dp)
    nxt = lax.rem(sec + 1, n_s)
    prv = lax.rem(sec + n_s - 1, n_s)
    right = lax.rem(dp + 1, n_d)
    left = lax.rem(dp + n_d - 1, n_d)
    opp = lax.rem(dp + 2, n_d)
    to_right = (sec, exp, right)
    to_left = (sec, exp, left)
    to_next = (nxt, exp, dp)
    to_prev = (prv, exp, dp)
    offs = sorted(range(1, n_y), key=lambda o: -min(o, n_y - o))
    last = steps - 1

    def row(o):
        return lax.rem(y + o, n_y)

    above = (sec, row(1) * CORES + core, dp)
    below = (sec, row(n_y - 1) * CORES + core, dp)
    first_sec = sec == 0
    last_sec = sec == n_s - 1

    barrier = pltpu.get_barrier_semaphore()

    def signal(target):
        pl.semaphore_signal(barrier, inc=1, device_id=target, device_id_type=MESH)

    for target in (to_right, to_left, sibling, above, below):
        signal(target)

    @pl.when(jnp.logical_not(last_sec))
    def _():
        signal(to_next)

    @pl.when(first_sec)
    def _():
        signal(to_prev)

    greeted = 5 + jnp.minimum(sec, 1) + sec // (n_s - 1)

    def tell(i, *targets):
        for target in targets:
            pl.semaphore_signal(ready.at[i], inc=1, device_id=target, device_id_type=MESH)

    def told(i, n):
        pl.semaphore_wait(ready.at[i], n)

    def ring(i):
        told(NEAR + i, 2)
        if i < 3:
            tell(NEAR + i + 1, above, below)

    loads = []

    def load(src, dst):
        copy = pltpu.make_async_copy(src, dst, load_sems.at[len(loads)])
        copy.start()
        loads.append(copy)
        return copy

    def at_cols(c):
        return pl.ds(pl.multiple_of(c * cols, cols), cols)

    def piece(c):
        return pl.ds(c * cols, cols)

    subs = range(n_c)
    mine = core * n_d + dp
    theirs = (1 - core) * n_d

    def own(x):
        return core * n_d + x

    load_w = [load(wg_h.at[0], wg.at[mine]), load(wu_h.at[0], wu.at[mine])]
    load_r = [load(routes_h, routes), load(gates_h, gates)]
    load_a = load(arr_h.at[0], inc.at[0])
    load_d = [load(wd_h.at[0, :, piece(q)], wd.at[mine, q]) for q in range(2)]
    load_c = load(cot_h, cot)
    load_g = load(gain_h, gain)
    load_f = load(fresh_h.at[0], fresh)

    def send_of(sem):
        firsts = (TOK, COT, CROSS, SWAP, HID, RET, RET + 7, PICK, BASE, BACK)
        if sem >= PART:
            return firsts.index(COT if sem < OVER else HID)
        return max(i for i, first in enumerate(firsts) if sem >= first)

    def remote(src, dst, sem, target):
        return pltpu.make_async_remote_copy(
            src_ref=src, dst_ref=dst, send_sem=send_sems.at[send_of(sem)],
            recv_sem=recv_sems.at[sem], device_id=target, device_id_type=MESH,
        )

    def got(ref, sem):
        remote(ref, ref, sem, sibling).wait_recv()

    def sent(ref, sem):
        remote(ref, ref, sem, sibling).wait_send()

    mats = (wg, wu)

    def w_copy(ref, m, i, target):
        return pltpu.make_async_remote_copy(
            src_ref=ref, dst_ref=ref, send_sem=w_send.at[m], recv_sem=w_recv.at[m, i],
            device_id=target, device_id_type=MESH,
        )

    def w_own(m):
        load_w[m].wait()
        ref = mats[m].at[mine]
        w_copy(ref, m, 0, to_right).start()
        w_copy(ref, m, 1, to_left).start()
        w_copy(ref, m, 3, sibling).start()

    def w_pass(m):
        w = mats[m]
        w_copy(w.at[own(left)], m, 0, sibling).wait_recv()
        w_copy(w.at[own(left), pl.ds(0, part_units)], m, 2, to_right).start()
        w_copy(w.at[own(left)], m, 3, sibling).start()
        w_copy(w.at[own(right)], m, 1, sibling).wait_recv()
        w_copy(w.at[own(right), pl.ds(part_units, part_units)], m, 2, to_left).start()
        w_copy(w.at[own(right)], m, 3, sibling).start()

    def w_last(m):
        ref = mats[m].at[own(opp)]
        w_copy(ref, m, 2, sibling).wait_recv()
        w_copy(ref, m, 4, sibling).start()

    def w_twin(m, far_one):
        if far_one:
            w_copy(mats[m].at[theirs + opp], m, 4, sibling).wait_recv()
        else:
            w_copy(mats[m].at[pl.ds(theirs, 3)], m, 3, sibling).wait_recv()

    def d_copy(ref, i, target):
        return pltpu.make_async_remote_copy(
            src_ref=ref, dst_ref=ref, send_sem=w_send.at[2], recv_sem=d_recv.at[i],
            device_id=target, device_id_type=MESH,
        )

    def d_own():
        for q in range(2):
            load_d[q].wait()
            d_copy(wd.at[mine, q], q, to_right).start()
            d_copy(wd.at[mine, q], 2 + q, to_left).start()
        d_copy(wd.at[mine], 6, sibling).start()

    def d_pass(q):
        d_copy(wd.at[own(left), q], q, sibling).wait_recv()
        d_copy(wd.at[own(left), q, pl.ds(0, part_units)], 4 + q, to_right).start()
        d_copy(wd.at[own(left), q], 7 + q, sibling).start()
        d_copy(wd.at[own(right), q], 2 + q, sibling).wait_recv()
        d_copy(wd.at[own(right), q, pl.ds(part_units, part_units)], 4 + q, to_left).start()
        d_copy(wd.at[own(right), q], 7 + q, sibling).start()

    def d_last(q):
        ref = wd.at[own(opp), q]
        d_copy(ref, 4 + q, sibling).wait_recv()
        d_copy(ref, 9 + q, sibling).start()

    def d_twin(name, q):
        if name == "own":
            d_copy(wd.at[theirs + dp], 6, sibling).wait_recv()
        elif name == "near":
            d_copy(wd.at[theirs + dp], 7 + q, sibling).wait_recv()
        else:
            d_copy(wd.at[theirs + opp, q], 9 + q, sibling).wait_recv()

    lane = lax.broadcasted_iota(jnp.int32, (used, rows), 0)
    lane_expert = lane >> 4
    lane_slot = lane & (SLOTS - 1)
    t_row = lax.broadcasted_iota(jnp.int32, (rows, rows), 0)
    t_col = lax.broadcasted_iota(jnp.int32, (rows, rows), 1)
    earlier_tok = jnp.where(t_row < t_col, 1.0, 0.0).astype(BF)

    def selection(k):
        naming = jnp.zeros((used, rows), F32)
        shares = jnp.zeros((used, rows), F32)
        for j in range(routes.shape[1]):
            hit = routes[0, j, k:k + 1, :] == lane_expert
            naming = jnp.where(hit, 1.0, naming)
            shares = shares + jnp.where(hit, gates[0, j].astype(F32)[k:k + 1, :], 0.0)
        places = mm(naming.astype(BF), earlier_tok)
        chosen = jnp.where(places == lane_slot.astype(F32), naming, 0.0)
        chosen = jnp.where(lane_slot < CAP, chosen, 0.0)
        return chosen.astype(BF), (chosen * shares).astype(BF)

    r_i = lax.broadcasted_iota(jnp.int32, (CAP * n_y, n_low), 0)
    c_i = lax.broadcasted_iota(jnp.int32, (CAP * n_y, n_low), 1)
    c_slot = c_i & 7
    shift = r_i - (c_i >> 3) * CAP - c_slot
    low_rows = jnp.where(shift == 0, 1.0, 0.0)
    tail_a = jnp.where((shift == 8) & (c_slot < 4), 1.0, 0.0)
    tail_b = jnp.where((shift == 4) & (c_slot >= 4), 1.0, 0.0)
    layout = jnp.concatenate([low_rows, tail_a, tail_b], axis=1).astype(BF)
    blank = jnp.zeros((n_low, half), BF)

    def swap(block):
        return jnp.concatenate([block[4:], block[:4]], axis=0)

    def fill(store, k, c, block):
        for f in range(flight):
            top = block[f * SLOTS:f * SLOTS + 8]
            bottom = block[f * SLOTS + 8:(f + 1) * SLOTS]
            store[k, c, f, :, :cols] = top.astype(BF)
            store[k, c, f, :, cols:] = (bottom[:, :half] + swap(bottom[:, half:])).astype(BF)

    def unpack(landing, *at):
        flat = landing[at].reshape(n_low, cols + half)
        tail = flat[:, cols:]
        stacked = jnp.concatenate(
            [
                flat[:, :cols],
                jnp.concatenate([tail, blank], axis=1),
                jnp.concatenate([blank, tail], axis=1),
            ],
            axis=0,
        )
        return mm(layout, stacked)

    def spread(store, landing, k, sem, targets, sub=0, n=None):
        n = n_c if n is None else n
        for o in targets:
            remote(
                store.at[k, pl.ds(sub, n), row(o) // PAIRS], landing.at[k, pl.ds(sub, n), y],
                sem, (sec, row(o) * CORES + core, dp),
            ).start()

    def keep(store, landing, k, sub, n):
        for q in range(n):
            landing[k, sub + q, y] = store[k, sub + q, y // PAIRS]

    def prepare(k, c):
        block = unpack(tokr, k, c)
        xg[c] = (block * gain[:, at_cols(c)]).astype(BF)
        return jnp.sum(block * block, axis=1, keepdims=True)

    def contract(parts, first, cores, which=(0, 1)):
        for c in cores:
            for i in which:
                w = mats[i]
                total = sum(
                    mm(xg[2 * ch + q], w[c * n_d + ch, :, q * cols:(q + 1) * cols], 1, 1)
                    for ch, q in parts
                )
                acc[i, c] = total if first else acc[i, c] + total

    def send_hidden(k):
        slot = hidr.at[k, mine]
        for x in (opp, right, left)[0 if k == last else 1:]:
            for c in range(CORES):
                there = y * CORES + c
                remote(hid_s.at[k, c], slot, HID + k, (sec, there, x)).start()
        remote(hid_s.at[k, 1 - core], slot, HID + k if k == last else OVER, sibling).start()
        hidr[k, mine] = hid_s[k, core]

    half_rows = CAP * n_y // 2

    def pass_hidden():
        got(hidr.at[0, pl.ds(0, 2 * CORES)], HID)
        for c in range(CORES):
            upper = hidr.at[0, c * n_d + left, pl.ds(0, half_rows)]
            lower = hidr.at[0, c * n_d + right, pl.ds(half_rows, half_rows)]
            remote(upper, upper, OVER, to_right).start()
            remote(lower, lower, OVER, to_left).start()

    def activate(k, squares, early):
        scale = lax.rsqrt(squares * (1.0 / width) + 0.5)
        for c in range(CORES):
            act_g = acc[0, c] * scale
            hid_s[k, c] = (act_g / (1.0 + jnp.exp(-act_g)) * (acc[1, c] * scale)).astype(BF)
        if early:
            send_hidden(k)
        for c in range(CORES):
            hp[c] = mm(layout, hid_s[k, c], 0, 0).astype(BF)

    def down(k, ch, qs, i, late=None):
        sub = 2 * ch + qs[0]
        for q in qs:
            rows_out = mm(hp[core], wd[own(ch), q])
            if late is not None and q == qs[0]:
                d_twin(late, q)
            rows_out = rows_out + mm(hp[1 - core], wd[theirs + ch, q])
            tail = rows_out[n_low:2 * n_low, :half] + rows_out[2 * n_low:, half:]
            rets[k, 2 * ch + q, :, :, :cols] = rows_out[:n_low].astype(BF).reshape(n_y, 8, cols)
            rets[k, 2 * ch + q, :, :, cols:] = tail.astype(BF).reshape(n_y, 8, half)
        there = sec if k == last else nxt
        span = pl.ds(sub, len(qs))
        for o in offs + ([] if k == last else [0]):
            remote(
                rets.at[k, span, row(o)], retr.at[k, span, y], RET + 7 * k + i,
                (there, row(o) * CORES + core, dp),
            ).start()
        if k == last:
            for q in qs:
                retr[k, 2 * ch + q, y] = rets[k, 2 * ch + q, y]

    row_8 = lax.broadcasted_iota(jnp.int32, (8, half), 0)

    def landed(k, ch, qs, i):
        n = n_y - 1 if k == last else n_y
        got(retr.at[k, pl.ds(2 * ch + qs[0], len(qs)), pl.ds(0, n)], RET + 7 * k + i)

    def combine(k, c, weights, inputs):
        tops = []
        for f in range(flight):
            total = sum(retr[k, c, f * PAIRS + p].astype(F32) for p in range(PAIRS))
            tail = total[:, cols:]
            tops.append(total[:, :cols])
            tops.append(jnp.concatenate(
                [jnp.where(row_8 < 4, tail, 0.0), jnp.where(row_8 < 4, swap(tail), 0.0)], axis=1
            ))
        mixed = jnp.concatenate(tops, axis=0)
        high = mixed.astype(BF)
        low = (mixed - high.astype(F32)).astype(BF)
        mixture = mm(weights, high, 0, 0) + mm(weights, low, 0, 0)
        return (inputs.astype(F32) + mixture).astype(BF)

    pl.semaphore_wait(barrier, greeted)
    w_own(0)
    w_own(1)
    tell(NEAR, above, below)
    tell(CROSSED, to_right, to_left)

    @pl.when(jnp.logical_not(first_sec))
    def _():
        tell(NEXT, to_prev)

    @pl.when(last_sec)
    def _():
        tell(WRAP, to_next)

    for copy in load_r:
        copy.wait()
    picks = [selection(0)]
    pick_s[...] = picks[0][1]
    load_a.wait()
    for c in subs:
        fill(toks, 0, c, mm(picks[0][0], inc[0, :, c * cols:(c + 1) * cols]))
    spread(toks, tokr, 0, TOK, (1, n_y - 1))
    ring(0)
    spread(toks, tokr, 0, TOK, (2, n_y - 2))
    told(CROSSED, 2)
    tell(TWIN, sibling)
    picks.append(selection(1))
    load_c.wait()
    for c in subs:
        fill(cots, 0, c, mm(picks[0][1], cot[0, 0, :, c * cols:(c + 1) * cols]))
    ring(1)
    spread(toks, tokr, 0, TOK, (3, n_y - 3))
    for c in subs:
        fill(cots, 1, c, mm(picks[1][1], cot[0, 1, :, c * cols:(c + 1) * cols]))
    ring(2)
    spread(toks, tokr, 0, TOK, (4,))

    @pl.when(jnp.logical_not(first_sec))
    def _():
        tell(RING, to_prev)

    spread(cots, cotr, 0, COT, offs)
    keep(toks, tokr, 0, 0, n_c)
    for k in range(steps):
        keep(cots, cotr, k, 0, n_c)
    load_f.wait()
    load_g.wait()

    items = (
        (dp, (0, 1)), (right, (0,)), (left, (0,)), (right, (1,)), (left, (1,)),
        (opp, (0,)), (opp, (1,)),
    )

    def enter(i, blocks):
        ch, qs = items[i]
        for q, block in zip(qs, blocks):
            inc[1, :, at_cols(2 * ch + q)] = block
            fill(toks, 1, 2 * ch + q, mm(picks[1][0], block))
        spread(toks, tokr, 1, TOK + 1 + i, offs, 2 * ch + qs[0], len(qs))
        keep(toks, tokr, 1, 2 * ch + qs[0], len(qs))

    @pl.when(first_sec)
    def _():
        for i, (ch, qs) in enumerate(items):
            enter(i, [fresh[:, at_cols(2 * ch + q)] for q in qs])

    @pl.when(jnp.logical_not(first_sec))
    def _():
        spread(cots, cotr, 1, COT + 1, offs)

    order = (dp, right, left, opp)

    def later(*blocks):
        @pl.when(first_sec)
        def _():
            for i in blocks:
                spread(cots, cotr, 1, PART + i, offs, 2 * order[i], 2)


    @pl.when(jnp.logical_not(last_sec))
    def _():
        told(NEXT, 1)

    remote(inc.at[0], base, BASE, to_next).start()
    remote(pick_s, pick_r, PICK, to_next).start()
    told(TWIN, 1)

    def settle(i):
        ch, qs = items[i]
        landed(0, ch, qs, i)
        results = []
        for q in qs:
            c = 2 * ch + q
            results.append(combine(0, c, pick_r[...], base[:, at_cols(c)]))
            back[c] = results[-1]
            remote(back.at[c], out.at[0, 0, :, at_cols(c)], BACK, to_prev).start()
        return results

    def relay(i):
        @pl.when(jnp.logical_not(first_sec))
        def _():
            enter(i, settle(i))

    def tok_in(i):
        ch, qs = items[i]
        got(tokr.at[1, pl.ds(2 * ch + qs[0], len(qs)), pl.ds(0, n_y - 1)], TOK + 1 + i)
        return sum(prepare(1, 2 * ch + q) for q in qs)

    def parts_of(*which):
        return [(items[i][0], q) for i in which for q in items[i][1]]

    near = parts_of(0, 1, 2, 3, 4)
    far = parts_of(5, 6)
    w_pass(0)
    got(tokr.at[0, pl.ds(0, n_c), pl.ds(0, n_y - 1)], TOK)
    squares = sum(prepare(0, c) for c in subs)
    w_pass(1)
    d_own()
    contract(near, True, (core,))
    w_twin(0, False)
    w_twin(1, False)
    contract(near, True, (1 - core,))
    w_last(0)
    contract(far, False, (core,), (0,))
    w_twin(0, True)
    contract(far, False, (1 - core,), (0,))
    w_last(1)
    contract(far, False, (core,), (1,))
    w_twin(1, True)
    contract(far, False, (1 - core,), (1,))
    activate(0, squares, False)
    ring(3)

    @pl.when(jnp.logical_not(last_sec))
    def _():
        told(RING, 1)

    down(0, dp, (0, 1), 0, "own")
    later(3)
    d_pass(0)
    d_twin("near", 0)
    down(0, right, (0,), 1)
    down(0, left, (0,), 2)
    later(1)
    got(base, BASE)
    got(pick_r, PICK)
    d_pass(1)
    relay(0)
    d_twin("near", 1)
    down(0, right, (1,), 3)
    down(0, left, (1,), 4)

    def hand(k, x):
        remote(
            cotr.at[k, pl.ds(2 * x, 2)], cotx.at[k, core, dp], CROSS + k, (sec, exp, x)
        ).start()

    def stay(k):
        for q in range(2):
            cotx[k, core, dp, q] = cotr[k, 2 * dp + q]

    def cross(k):
        got(cotr.at[k, pl.ds(0, n_c), pl.ds(0, n_y - 1)], COT + k)
        for x in (opp, right, left):
            hand(k, x)
        stay(k)

    def cross_part(i):
        got(cotr.at[1, pl.ds(2 * order[i], 2), pl.ds(0, n_y - 1)], PART + i)
        if i:
            hand(1, order[i])
        else:
            stay(1)

    d_last(0)
    send_hidden(0)
    cross(0)
    relay(1)
    d_last(1)
    down(0, opp, (0,), 5, "far")
    down(0, opp, (1,), 6, "far")
    later(2, 0)

    @pl.when(jnp.logical_not(first_sec))
    def _():
        cross(1)

    relay(2)
    squares = tok_in(0)
    contract(parts_of(0), True, (0, 1))
    relay(3)
    relay(4)
    relay(5)
    relay(6)
    squares = squares + tok_in(1)
    contract(parts_of(1), False, (0, 1))

    @pl.when(jnp.logical_not(first_sec))
    def _():
        pass_hidden()

    squares = squares + tok_in(2)
    contract(parts_of(2), False, (0, 1))
    squares = squares + tok_in(3) + tok_in(4)
    contract(parts_of(3, 4), False, (0, 1))
    squares = squares + tok_in(5)
    contract(parts_of(5), False, (0, 1))
    squares = squares + tok_in(6)
    contract(parts_of(6), False, (0, 1))
    activate(1, squares, True)
    for i, ch in enumerate(order):
        down(1, ch, (0, 1), i)

    def results():
        for i, ch in enumerate(order):
            landed(1, ch, (0, 1), i)
            for q in range(2):
                c = 2 * ch + q
                out[0, 1, :, at_cols(c)] = combine(1, c, picks[1][1], inc[1, :, at_cols(c)])

    @pl.when(first_sec)
    def _():
        pass_hidden()
        for i in (3, 1, 2, 0):
            cross_part(i)

    @pl.when(first_sec)
    def _():
        told(WRAP, 1)
        for i in range(len(items)):
            settle(i)

    for k in range(steps):
        got(cotx.at[k, core, pl.ds(0, n_d - 1)], CROSS + k)
        remote(cotx.at[k, core], cotx.at[k, core], SWAP + k, sibling).start()
        got(cotx.at[k, 0], SWAP + k)
        if k == last:
            got(hidr.at[k, pl.ds(0, CORES * n_d - 1)], HID + k)
        else:
            got(hidr.at[k, pl.ds(0, CORES + 1)], OVER)
        total = 0.0
        for c in range(CORES):
            rows_cot = jnp.concatenate(
                [
                    jnp.concatenate(
                        [unpack(cotx, k, c, x, q).astype(BF) for q in range(2)], axis=1
                    )
                    for x in range(n_d)
                ],
                axis=0,
            )
            rows_hid = hidr[k, pl.ds(c * n_d, n_d)].reshape(n_d * CAP * n_y, units)
            total = total + mm(rows_hid, rows_cot, 0, 0)
        grad[0] = total if k == 0 else grad[0] + total
        if k == 0:

            @pl.when(first_sec)
            def _():
                results()


    @pl.when(jnp.logical_not(first_sec))
    def _():
        results()

    got(back, BACK)
    for m, w in enumerate(mats + (wd,)):
        ref = w.at[pl.ds(0, CORES * n_d - 1)]
        pltpu.make_async_remote_copy(
            src_ref=ref, dst_ref=ref, send_sem=w_send.at[m], recv_sem=w_recv.at[0, 0],
            device_id=sibling, device_id_type=MESH,
        ).wait_send()
    both, every, others = pl.ds(0, steps), pl.ds(0, n_c), pl.ds(0, n_y - 1)
    sent(tokr.at[both, every, others], TOK)
    sent(cotr.at[both, every, others], COT)
    sent(cotx.at[both, 0, pl.ds(0, n_d - 1)], CROSS)
    sent(cotx.at[both, 0], SWAP)
    sent(hidr.at[both, pl.ds(0, CORES * n_d - 1)], HID)
    sent(retr.at[0], RET)
    sent(retr.at[1, every, others], RET + 7)
    sent(pick_s, PICK)
    sent(base, BASE)
    sent(back, BACK)


def finish(out_in, grad_in, out, grad, sems):
    pieces = ((out_in, out), (grad_in, grad))
    copies = [pltpu.make_async_copy(src, dst, sems.at[i]) for i, (src, dst) in enumerate(pieces)]
    for copy in copies:
        copy.start()
    for copy in copies:
        copy.wait()


def local(sizes, arrivals, fresh, routes, gates, cotangent, norm_gain, w_gate, w_up, w_down):
    n_s, n_e, n_d = sizes
    steps = routes.shape[1]
    tok_rows, width = arrivals.shape[1:]
    units, cols = w_gate.shape[1:]
    flight = n_e // SPLIT
    n_y = n_e // CORES
    n_c = 2 * n_d
    rows = CAP * n_y
    used = flight * SLOTS
    sub = cols // 2
    packed = sub + sub // 2
    hbm = pl.BlockSpec(memory_space=pltpu.HBM)
    held = pl.BlockSpec(memory_space=pltpu.VMEM)

    def vmem(*shape, kind=BF):
        return pltpu.VMEM(shape, kind)

    dma = pltpu.SemaphoreType.DMA
    made = pl.pallas_call(
        functools.partial(kernel, n_s, n_e, n_d, steps),
        out_shape=(
            pltpu.VMEM((1, steps, tok_rows, width), BF),
            pltpu.VMEM((1, units, cols), F32),
        ),
        in_specs=[hbm] * 9,
        out_specs=(held, held),
        scratch_shapes=[
            vmem(CORES * n_d, units, cols),
            vmem(CORES * n_d, units, cols),
            vmem(CORES * n_d, 2, units, sub),
            vmem(1, routes.shape[3], steps, tok_rows, kind=jnp.int32),
            vmem(1, routes.shape[3], steps, tok_rows),
            vmem(1, width, kind=F32),
            vmem(*cotangent.shape),
            vmem(tok_rows, width),
            vmem(steps, tok_rows, width),
            vmem(tok_rows, width),
            vmem(steps, n_c, flight, 8, packed),
            vmem(steps, n_c, n_y, 8, packed),
            vmem(steps, n_c, flight, 8, packed),
            vmem(steps, n_c, n_y, 8, packed),
            vmem(steps, CORES, n_d, 2, n_y, 8, packed),
            vmem(n_c, rows, sub),
            vmem(2, CORES, rows, units, kind=F32),
            vmem(steps, CORES, rows, units),
            vmem(steps, CORES * n_d, rows, units),
            vmem(CORES, 24 * n_y, units),
            vmem(steps, n_c, n_y, 8, packed),
            vmem(steps, n_c, n_y, 8, packed),
            vmem(used, tok_rows),
            vmem(used, tok_rows),
            vmem(n_c, tok_rows, sub),
            dma((10,)),
            dma((3,)),
            dma((2, 5)),
            dma((11,)),
            dma((SENDS,)),
            dma((SEMS,)),
            pltpu.SemaphoreType.REGULAR((READY,)),
        ],
        compiler_params=pltpu.CompilerParams(
            collective_id=0, has_side_effects=True, vmem_limit_bytes=64240 * 1024
        ),
    )(
        arrivals, fresh, jnp.transpose(routes, (0, 3, 1, 2)),
        jnp.transpose(gates, (0, 3, 1, 2)), cotangent,
        norm_gain, w_gate, w_up, w_down,
    )
    return pl.pallas_call(
        finish,
        out_shape=tuple(jax.ShapeDtypeStruct(m.shape, m.dtype) for m in made),
        in_specs=[held] * 2,
        out_specs=(hbm, hbm),
        scratch_shapes=[pltpu.SemaphoreType.DMA((2,))],
        compiler_params=pltpu.CompilerParams(vmem_limit_bytes=4096 * 1024),
    )(*made)


def solution(mesh):
    placed = (
        P("section", ("expert", "dp"), None),
        P(None, ("expert", "dp"), None),
        P("section", None, ("expert", "dp"), None),
        P("section", None, ("expert", "dp"), None),
        P("section", None, ("expert", "dp"), None),
        P("section", None),
        P("section", "expert", "dp"),
        P("section", "expert", "dp"),
        P("section", "expert", "dp"),
    )
    sizes = (mesh.shape["section"], mesh.shape["expert"], mesh.shape["dp"])
    return jax.shard_map(
        functools.partial(local, sizes),
        mesh=mesh,
        in_specs=placed,
        out_specs=(P("section", None, ("expert", "dp"), None), P("section", "expert", "dp")),
        check_vma=False,
    )
```

```python
import functools

import jax
import jax.numpy as jnp
from jax import lax
from jax.experimental import pallas as pl
from jax.experimental.pallas import tpu as pltpu
from jax.sharding import PartitionSpec as P

SPLIT = 4
CAP = 12
SLOTS = 16
CORES = 2
PAIRS = SPLIT // CORES
MESH = pl.DeviceIdType.MESH
BF = jnp.bfloat16
F32 = jnp.float32

TOK, COT, CROSS, SWAP, HID, RET, PICK, BASE, BACK, PART, OVER, SEMS = 0, 8, 10, 12, 14, 16, 27, 28, 29, 30, 34, 35
SENDS = 10
NEAR, NEXT, RING, WRAP, CROSSED, TWIN, READY = 0, 4, 5, 6, 7, 8, 9


def mm(a, b, ca=1, cb=0):
    return lax.dot_general(a, b, (((ca,), (cb,)), ((), ())), preferred_element_type=F32)


def kernel(
    n_s, n_e, n_d, steps,
    arr_h, fresh_h, routes_h, gates_h, cot_h, gain_h, wg_h, wu_h, wd_h,
    out, grad,
    wg, wu, wd, routes, gates, gain, cot, fresh, inc, base,
    toks, tokr, cots, cotr, cotx, xg, acc, hid_s, hidr, hp, rets, retr,
    pick_s, pick_r, back,
    load_sems, w_send, g_recv, h_recv, send_sems, recv_sems, ready,
):
    sec = lax.axis_index("section")
    exp = lax.axis_index("expert")
    dp = lax.axis_index("dp")
    n_y = n_e // CORES
    flight = n_e // SPLIT
    n_c, rows, cols = back.shape
    half = cols // 2
    units = wd.shape[2]
    part_units = units // 2
    width = cols * n_c
    used = flight * SLOTS
    n_low = 8 * n_y
    core = lax.rem(exp, CORES)
    y = exp // CORES
    sibling = (sec, exp + 1 - 2 * core, dp)
    nxt = lax.rem(sec + 1, n_s)
    prv = lax.rem(sec + n_s - 1, n_s)
    right = lax.rem(dp + 1, n_d)
    left = lax.rem(dp + n_d - 1, n_d)
    opp = lax.rem(dp + 2, n_d)
    to_right = (sec, exp, right)
    to_left = (sec, exp, left)
    to_next = (nxt, exp, dp)
    to_prev = (prv, exp, dp)
    offs = sorted(range(1, n_y), key=lambda o: -min(o, n_y - o))
    last = steps - 1

    def row(o):
        return lax.rem(y + o, n_y)

    above = (sec, row(1) * CORES + core, dp)
    below = (sec, row(n_y - 1) * CORES + core, dp)
    first_sec = sec == 0
    last_sec = sec == n_s - 1

    barrier = pltpu.get_barrier_semaphore()

    def signal(target):
        pl.semaphore_signal(barrier, inc=1, device_id=target, device_id_type=MESH)

    for target in (to_right, to_left, sibling, above, below):
        signal(target)

    @pl.when(jnp.logical_not(last_sec))
    def _():
        signal(to_next)

    @pl.when(first_sec)
    def _():
        signal(to_prev)

    greeted = 5 + jnp.minimum(sec, 1) + sec // (n_s - 1)

    def tell(i, *targets):
        for target in targets:
            pl.semaphore_signal(ready.at[i], inc=1, device_id=target, device_id_type=MESH)

    def told(i, n):
        pl.semaphore_wait(ready.at[i], n)

    def ring(i):
        told(NEAR + i, 2)
        if i < 3:
            tell(NEAR + i + 1, above, below)

    loads = []

    def load(src, dst):
        copy = pltpu.make_async_copy(src, dst, load_sems.at[len(loads)])
        copy.start()
        loads.append(copy)
        return copy

    def at_cols(c):
        return pl.ds(pl.multiple_of(c * cols, cols), cols)

    def piece(c):
        return pl.ds(c * cols, cols)

    subs = range(n_c)
    mine = core * n_d + dp
    theirs = (1 - core) * n_d

    def own(x):
        return core * n_d + x

    load_w = load(wg_h.at[0], wg.at[mine])
    load_u = [load(wu_h.at[0, :, piece(q)], wu.at[mine, q]) for q in range(2)]
    load_r = [load(routes_h, routes), load(gates_h, gates)]
    load_a = load(arr_h.at[0], inc.at[0])
    load_d = [load(wd_h.at[0, :, piece(q)], wd.at[mine, q]) for q in range(2)]
    load_c = load(cot_h, cot)
    load_g = load(gain_h, gain)
    load_f = load(fresh_h.at[0], fresh)

    def send_of(sem):
        firsts = (TOK, COT, CROSS, SWAP, HID, RET, RET + 7, PICK, BASE, BACK)
        if sem >= PART:
            return firsts.index(COT if sem < OVER else HID)
        return max(i for i, first in enumerate(firsts) if sem >= first)

    def remote(src, dst, sem, target):
        return pltpu.make_async_remote_copy(
            src_ref=src, dst_ref=dst, send_sem=send_sems.at[send_of(sem)],
            recv_sem=recv_sems.at[sem], device_id=target, device_id_type=MESH,
        )

    def got(ref, sem):
        remote(ref, ref, sem, sibling).wait_recv()

    def sent(ref, sem):
        remote(ref, ref, sem, sibling).wait_send()

    def g_copy(ref, i, target):
        return pltpu.make_async_remote_copy(
            src_ref=ref, dst_ref=ref, send_sem=w_send.at[0], recv_sem=g_recv.at[i],
            device_id=target, device_id_type=MESH,
        )

    def g_own():
        load_w.wait()
        ref = wg.at[mine]
        g_copy(ref, 0, to_right).start()
        g_copy(ref, 1, to_left).start()
        g_copy(ref, 3, sibling).start()

    def g_pass():
        g_copy(wg.at[own(left)], 0, sibling).wait_recv()
        g_copy(wg.at[own(left), pl.ds(0, part_units)], 2, to_right).start()
        g_copy(wg.at[own(left)], 3, sibling).start()
        g_copy(wg.at[own(right)], 1, sibling).wait_recv()
        g_copy(wg.at[own(right), pl.ds(part_units, part_units)], 2, to_left).start()
        g_copy(wg.at[own(right)], 3, sibling).start()

    def g_last():
        ref = wg.at[own(opp)]
        g_copy(ref, 2, sibling).wait_recv()
        g_copy(ref, 4, sibling).start()

    def g_twin(far_one):
        if far_one:
            g_copy(wg.at[theirs + opp], 4, sibling).wait_recv()
        else:
            g_copy(wg.at[pl.ds(theirs, 3)], 3, sibling).wait_recv()

    halves = (wu, wd)

    def h_copy(ref, m, i, target):
        return pltpu.make_async_remote_copy(
            src_ref=ref, dst_ref=ref, send_sem=w_send.at[1 + m], recv_sem=h_recv.at[m, i],
            device_id=target, device_id_type=MESH,
        )

    def h_own(m):
        w = halves[m]
        for q in range(2):
            (load_u, load_d)[m][q].wait()
            h_copy(w.at[mine, q], m, q, to_right).start()
            h_copy(w.at[mine, q], m, 2 + q, to_left).start()
        h_copy(w.at[mine], m, 6, sibling).start()

    def h_pass(m, q):
        w = halves[m]
        h_copy(w.at[own(left), q], m, q, sibling).wait_recv()
        h_copy(w.at[own(left), q, pl.ds(0, part_units)], m, 4 + q, to_right).start()
        h_copy(w.at[own(left), q], m, 7 + q, sibling).start()
        h_copy(w.at[own(right), q], m, 2 + q, sibling).wait_recv()
        h_copy(w.at[own(right), q, pl.ds(part_units, part_units)], m, 4 + q, to_left).start()
        h_copy(w.at[own(right), q], m, 7 + q, sibling).start()

    def h_last(m, q):
        ref = halves[m].at[own(opp), q]
        h_copy(ref, m, 4 + q, sibling).wait_recv()
        h_copy(ref, m, 9 + q, sibling).start()

    def h_twin(m, name, q):
        w = halves[m]
        if name == "own":
            h_copy(w.at[theirs + dp], m, 6, sibling).wait_recv()
        elif name == "near":
            h_copy(w.at[theirs + dp], m, 7 + q, sibling).wait_recv()
        else:
            h_copy(w.at[theirs + opp, q], m, 9 + q, sibling).wait_recv()

    lane = lax.broadcasted_iota(jnp.int32, (used, rows), 0)
    lane_expert = lane >> 4
    lane_slot = lane & (SLOTS - 1)
    t_row = lax.broadcasted_iota(jnp.int32, (rows, rows), 0)
    t_col = lax.broadcasted_iota(jnp.int32, (rows, rows), 1)
    earlier_tok = jnp.where(t_row < t_col, 1.0, 0.0).astype(BF)

    def selection(k):
        naming = jnp.zeros((used, rows), F32)
        shares = jnp.zeros((used, rows), F32)
        for j in range(routes.shape[1]):
            hit = routes[0, j, k:k + 1, :] == lane_expert
            naming = jnp.where(hit, 1.0, naming)
            shares = shares + jnp.where(hit, gates[0, j].astype(F32)[k:k + 1, :], 0.0)
        places = mm(naming.astype(BF), earlier_tok)
        chosen = jnp.where(places == lane_slot.astype(F32), naming, 0.0)
        chosen = jnp.where(lane_slot < CAP, chosen, 0.0)
        return chosen.astype(BF), (chosen * shares).astype(BF)

    r_i = lax.broadcasted_iota(jnp.int32, (CAP * n_y, n_low), 0)
    c_i = lax.broadcasted_iota(jnp.int32, (CAP * n_y, n_low), 1)
    c_slot = c_i & 7
    shift = r_i - (c_i >> 3) * CAP - c_slot
    low_rows = jnp.where(shift == 0, 1.0, 0.0)
    tail_a = jnp.where((shift == 8) & (c_slot < 4), 1.0, 0.0)
    tail_b = jnp.where((shift == 4) & (c_slot >= 4), 1.0, 0.0)
    layout = jnp.concatenate([low_rows, tail_a, tail_b], axis=1).astype(BF)
    blank = jnp.zeros((n_low, half), BF)

    def swap(block):
        return jnp.concatenate([block[4:], block[:4]], axis=0)

    def fill(store, k, c, block):
        for f in range(flight):
            top = block[f * SLOTS:f * SLOTS + 8]
            bottom = block[f * SLOTS + 8:(f + 1) * SLOTS]
            store[k, c, f, :, :cols] = top.astype(BF)
            store[k, c, f, :, cols:] = (bottom[:, :half] + swap(bottom[:, half:])).astype(BF)

    def unpack(landing, *at):
        flat = landing[at].reshape(n_low, cols + half)
        tail = flat[:, cols:]
        stacked = jnp.concatenate(
            [
                flat[:, :cols],
                jnp.concatenate([tail, blank], axis=1),
                jnp.concatenate([blank, tail], axis=1),
            ],
            axis=0,
        )
        return mm(layout, stacked)

    def spread(store, landing, k, sem, targets, sub=0, n=None):
        n = n_c if n is None else n
        for o in targets:
            remote(
                store.at[k, pl.ds(sub, n), row(o) // PAIRS], landing.at[k, pl.ds(sub, n), y],
                sem, (sec, row(o) * CORES + core, dp),
            ).start()

    def keep(store, landing, k, sub, n):
        for q in range(n):
            landing[k, sub + q, y] = store[k, sub + q, y // PAIRS]

    def prepare(k, c):
        block = unpack(tokr, k, c)
        xg[c] = (block * gain[:, at_cols(c)]).astype(BF)
        return jnp.sum(block * block, axis=1, keepdims=True)

    def contract(parts, first, cores, which=(0, 1)):
        for c in cores:
            for i in which:
                total = 0.0
                for ch, q in parts:
                    at = c * n_d + ch
                    w = wu[at, q] if i else wg[at, :, q * cols:(q + 1) * cols]
                    total = total + mm(xg[2 * ch + q], w, 1, 1)
                acc[i, c] = total if first else acc[i, c] + total

    def send_hidden(k):
        slot = hidr.at[k, mine]
        for x in (opp, right, left)[0 if k == last else 1:]:
            for c in range(CORES):
                there = y * CORES + c
                remote(hid_s.at[k, c], slot, HID + k, (sec, there, x)).start()
        remote(hid_s.at[k, 1 - core], slot, HID + k if k == last else OVER, sibling).start()
        hidr[k, mine] = hid_s[k, core]

    half_rows = CAP * n_y // 2

    def pass_hidden():
        got(hidr.at[0, pl.ds(0, 2 * CORES)], HID)
        for c in range(CORES):
            upper = hidr.at[0, c * n_d + left, pl.ds(0, half_rows)]
            lower = hidr.at[0, c * n_d + right, pl.ds(half_rows, half_rows)]
            remote(upper, upper, OVER, to_right).start()
            remote(lower, lower, OVER, to_left).start()

    def activate(k, squares, early):
        scale = lax.rsqrt(squares * (1.0 / width) + 0.5)
        for c in range(CORES):
            act_g = acc[0, c] * scale
            hid_s[k, c] = (act_g / (1.0 + jnp.exp(-act_g)) * (acc[1, c] * scale)).astype(BF)
        if early:
            send_hidden(k)
        for c in range(CORES):
            hp[c] = mm(layout, hid_s[k, c], 0, 0).astype(BF)

    def down(k, ch, qs, i, late=None):
        sub = 2 * ch + qs[0]
        for q in qs:
            rows_out = mm(hp[core], wd[own(ch), q])
            if late is not None and q == qs[0]:
                h_twin(1, late, q)
            rows_out = rows_out + mm(hp[1 - core], wd[theirs + ch, q])
            tail = rows_out[n_low:2 * n_low, :half] + rows_out[2 * n_low:, half:]
            rets[k, 2 * ch + q, :, :, :cols] = rows_out[:n_low].astype(BF).reshape(n_y, 8, cols)
            rets[k, 2 * ch + q, :, :, cols:] = tail.astype(BF).reshape(n_y, 8, half)
        there = sec if k == last else nxt
        span = pl.ds(sub, len(qs))
        for o in offs + ([] if k == last else [0]):
            remote(
                rets.at[k, span, row(o)], retr.at[k, span, y], RET + 7 * k + i,
                (there, row(o) * CORES + core, dp),
            ).start()
        if k == last:
            for q in qs:
                retr[k, 2 * ch + q, y] = rets[k, 2 * ch + q, y]

    row_8 = lax.broadcasted_iota(jnp.int32, (8, half), 0)

    def landed(k, ch, qs, i):
        n = n_y - 1 if k == last else n_y
        got(retr.at[k, pl.ds(2 * ch + qs[0], len(qs)), pl.ds(0, n)], RET + 7 * k + i)

    def combine(k, c, weights, inputs):
        tops = []
        for f in range(flight):
            total = sum(retr[k, c, f * PAIRS + p].astype(F32) for p in range(PAIRS))
            tail = total[:, cols:]
            tops.append(total[:, :cols])
            tops.append(jnp.concatenate(
                [jnp.where(row_8 < 4, tail, 0.0), jnp.where(row_8 < 4, swap(tail), 0.0)], axis=1
            ))
        mixed = jnp.concatenate(tops, axis=0)
        high = mixed.astype(BF)
        low = (mixed - high.astype(F32)).astype(BF)
        mixture = mm(weights, high, 0, 0) + mm(weights, low, 0, 0)
        return (inputs.astype(F32) + mixture).astype(BF)

    pl.semaphore_wait(barrier, greeted)
    g_own()
    h_own(0)
    tell(NEAR, above, below)
    tell(CROSSED, to_right, to_left)

    @pl.when(jnp.logical_not(first_sec))
    def _():
        tell(NEXT, to_prev)

    @pl.when(last_sec)
    def _():
        tell(WRAP, to_next)

    for copy in load_r:
        copy.wait()
    picks = [selection(0)]
    pick_s[...] = picks[0][1]
    load_a.wait()
    for c in subs:
        fill(toks, 0, c, mm(picks[0][0], inc[0, :, c * cols:(c + 1) * cols]))
    spread(toks, tokr, 0, TOK, (1, n_y - 1))
    ring(0)
    spread(toks, tokr, 0, TOK, (2, n_y - 2))
    told(CROSSED, 2)
    tell(TWIN, sibling)
    picks.append(selection(1))
    load_c.wait()
    for c in subs:
        fill(cots, 0, c, mm(picks[0][1], cot[0, 0, :, c * cols:(c + 1) * cols]))
    ring(1)
    spread(toks, tokr, 0, TOK, (3, n_y - 3))
    for c in subs:
        fill(cots, 1, c, mm(picks[1][1], cot[0, 1, :, c * cols:(c + 1) * cols]))
    ring(2)
    spread(toks, tokr, 0, TOK, (4,))

    @pl.when(jnp.logical_not(first_sec))
    def _():
        tell(RING, to_prev)

    spread(cots, cotr, 0, COT, offs)
    keep(toks, tokr, 0, 0, n_c)
    for k in range(steps):
        keep(cots, cotr, k, 0, n_c)
    load_f.wait()
    load_g.wait()

    items = (
        (dp, (0, 1)), (right, (0,)), (left, (0,)), (right, (1,)), (left, (1,)),
        (opp, (0,)), (opp, (1,)),
    )

    def enter(i, blocks):
        ch, qs = items[i]
        for q, block in zip(qs, blocks):
            inc[1, :, at_cols(2 * ch + q)] = block
            fill(toks, 1, 2 * ch + q, mm(picks[1][0], block))
        spread(toks, tokr, 1, TOK + 1 + i, offs, 2 * ch + qs[0], len(qs))
        keep(toks, tokr, 1, 2 * ch + qs[0], len(qs))

    @pl.when(first_sec)
    def _():
        for i, (ch, qs) in enumerate(items):
            enter(i, [fresh[:, at_cols(2 * ch + q)] for q in qs])

    @pl.when(jnp.logical_not(first_sec))
    def _():
        spread(cots, cotr, 1, COT + 1, offs)

    order = (dp, right, left, opp)

    def later(*blocks):
        @pl.when(first_sec)
        def _():
            for i in blocks:
                spread(cots, cotr, 1, PART + i, offs, 2 * order[i], 2)


    @pl.when(jnp.logical_not(last_sec))
    def _():
        told(NEXT, 1)

    remote(inc.at[0], base, BASE, to_next).start()
    remote(pick_s, pick_r, PICK, to_next).start()
    told(TWIN, 1)

    def settle(i):
        ch, qs = items[i]
        landed(0, ch, qs, i)
        results = []
        for q in qs:
            c = 2 * ch + q
            results.append(combine(0, c, pick_r[...], base[:, at_cols(c)]))
            back[c] = results[-1]
            remote(back.at[c], out.at[0, 0, :, at_cols(c)], BACK, to_prev).start()
        return results

    def relay(i):
        @pl.when(jnp.logical_not(first_sec))
        def _():
            enter(i, settle(i))

    def tok_in(i):
        ch, qs = items[i]
        got(tokr.at[1, pl.ds(2 * ch + qs[0], len(qs)), pl.ds(0, n_y - 1)], TOK + 1 + i)
        return sum(prepare(1, 2 * ch + q) for q in qs)

    def parts_of(*which):
        return [(items[i][0], q) for i in which for q in items[i][1]]

    near = parts_of(0, 1, 2, 3, 4)
    far = parts_of(5, 6)
    g_pass()
    got(tokr.at[0, pl.ds(0, n_c), pl.ds(0, n_y - 1)], TOK)
    squares = sum(prepare(0, c) for c in subs)
    h_pass(0, 0)
    h_pass(0, 1)
    h_own(1)
    contract(near, True, (core,))
    g_twin(False)
    h_twin(0, "own", 0)
    h_twin(0, "near", 0)
    h_twin(0, "near", 1)
    contract(near, True, (1 - core,))
    g_last()
    contract(far, False, (core,), (0,))
    g_twin(True)
    contract(far, False, (1 - core,), (0,))
    h_last(0, 0)
    contract(parts_of(5), False, (core,), (1,))
    h_last(0, 1)
    contract(parts_of(6), False, (core,), (1,))
    h_twin(0, "far", 0)
    contract(parts_of(5), False, (1 - core,), (1,))
    h_twin(0, "far", 1)
    contract(parts_of(6), False, (1 - core,), (1,))
    activate(0, squares, False)
    ring(3)

    @pl.when(jnp.logical_not(last_sec))
    def _():
        told(RING, 1)

    down(0, dp, (0, 1), 0, "own")
    later(3)
    h_pass(1, 0)
    h_twin(1, "near", 0)
    down(0, right, (0,), 1)
    down(0, left, (0,), 2)
    later(1)
    got(base, BASE)
    got(pick_r, PICK)
    h_pass(1, 1)
    relay(0)
    h_twin(1, "near", 1)
    down(0, right, (1,), 3)
    down(0, left, (1,), 4)

    def hand(k, x):
        remote(
            cotr.at[k, pl.ds(2 * x, 2)], cotx.at[k, core, dp], CROSS + k, (sec, exp, x)
        ).start()

    def stay(k):
        for q in range(2):
            cotx[k, core, dp, q] = cotr[k, 2 * dp + q]

    def cross(k):
        got(cotr.at[k, pl.ds(0, n_c), pl.ds(0, n_y - 1)], COT + k)
        for x in (opp, right, left):
            hand(k, x)
        stay(k)

    def cross_part(i):
        got(cotr.at[1, pl.ds(2 * order[i], 2), pl.ds(0, n_y - 1)], PART + i)
        if i:
            hand(1, order[i])
        else:
            stay(1)

    h_last(1, 0)
    send_hidden(0)
    cross(0)
    relay(1)
    h_last(1, 1)
    down(0, opp, (0,), 5, "far")
    down(0, opp, (1,), 6, "far")
    later(2, 0)

    @pl.when(jnp.logical_not(first_sec))
    def _():
        cross(1)

    relay(2)
    squares = tok_in(0)
    contract(parts_of(0), True, (0, 1))
    relay(3)
    relay(4)
    relay(5)
    relay(6)
    squares = squares + tok_in(1)
    contract(parts_of(1), False, (0, 1))

    @pl.when(jnp.logical_not(first_sec))
    def _():
        pass_hidden()

    squares = squares + tok_in(2)
    contract(parts_of(2), False, (0, 1))
    squares = squares + tok_in(3) + tok_in(4)
    contract(parts_of(3, 4), False, (0, 1))
    squares = squares + tok_in(5)
    contract(parts_of(5), False, (0, 1))
    squares = squares + tok_in(6)
    contract(parts_of(6), False, (0, 1))
    activate(1, squares, True)
    ends = tuple((ch, (0, 1)) for ch in order)
    for i, (ch, qs) in enumerate(ends):
        down(1, ch, qs, i)

    def results():
        for i, (ch, qs) in enumerate(ends):
            landed(1, ch, qs, i)
            for q in qs:
                c = 2 * ch + q
                out[0, 1, :, at_cols(c)] = combine(1, c, picks[1][1], inc[1, :, at_cols(c)])

    @pl.when(first_sec)
    def _():
        pass_hidden()
        for i in (3, 1, 2, 0):
            cross_part(i)

    @pl.when(first_sec)
    def _():
        told(WRAP, 1)
        for i in range(len(items)):
            settle(i)

    for k in range(steps):
        got(cotx.at[k, core, pl.ds(0, n_d - 1)], CROSS + k)
        remote(cotx.at[k, core], cotx.at[k, core], SWAP + k, sibling).start()
        got(cotx.at[k, 0], SWAP + k)
        if k == last:
            got(hidr.at[k, pl.ds(0, CORES * n_d - 1)], HID + k)
        else:
            got(hidr.at[k, pl.ds(0, CORES + 1)], OVER)
        total = 0.0
        for c in range(CORES):
            rows_cot = jnp.concatenate(
                [
                    jnp.concatenate(
                        [unpack(cotx, k, c, x, q).astype(BF) for q in range(2)], axis=1
                    )
                    for x in range(n_d)
                ],
                axis=0,
            )
            rows_hid = hidr[k, pl.ds(c * n_d, n_d)].reshape(n_d * CAP * n_y, units)
            total = total + mm(rows_hid, rows_cot, 0, 0)
        grad[0] = total if k == 0 else grad[0] + total
        if k == 0:

            @pl.when(first_sec)
            def _():
                results()


    @pl.when(jnp.logical_not(first_sec))
    def _():
        results()

    got(back, BACK)
    for m, w in enumerate((wg, wu, wd)):
        ref = w.at[pl.ds(0, CORES * n_d - 1)]
        pltpu.make_async_remote_copy(
            src_ref=ref, dst_ref=ref, send_sem=w_send.at[m], recv_sem=g_recv.at[0],
            device_id=sibling, device_id_type=MESH,
        ).wait_send()
    both, every, others = pl.ds(0, steps), pl.ds(0, n_c), pl.ds(0, n_y - 1)
    sent(tokr.at[both, every, others], TOK)
    sent(cotr.at[both, every, others], COT)
    sent(cotx.at[both, 0, pl.ds(0, n_d - 1)], CROSS)
    sent(cotx.at[both, 0], SWAP)
    sent(hidr.at[both, pl.ds(0, CORES * n_d - 1)], HID)
    sent(retr.at[0], RET)
    sent(retr.at[1, every, others], RET + 7)
    sent(pick_s, PICK)
    sent(base, BASE)
    sent(back, BACK)


def finish(out_in, grad_in, out, grad, sems):
    pieces = ((out_in, out), (grad_in, grad))
    copies = [pltpu.make_async_copy(src, dst, sems.at[i]) for i, (src, dst) in enumerate(pieces)]
    for copy in copies:
        copy.start()
    for copy in copies:
        copy.wait()


def local(sizes, arrivals, fresh, routes, gates, cotangent, norm_gain, w_gate, w_up, w_down):
    n_s, n_e, n_d = sizes
    steps = routes.shape[1]
    tok_rows, width = arrivals.shape[1:]
    units, cols = w_gate.shape[1:]
    flight = n_e // SPLIT
    n_y = n_e // CORES
    n_c = 2 * n_d
    rows = CAP * n_y
    used = flight * SLOTS
    sub = cols // 2
    packed = sub + sub // 2
    hbm = pl.BlockSpec(memory_space=pltpu.HBM)
    held = pl.BlockSpec(memory_space=pltpu.VMEM)

    def vmem(*shape, kind=BF):
        return pltpu.VMEM(shape, kind)

    dma = pltpu.SemaphoreType.DMA
    made = pl.pallas_call(
        functools.partial(kernel, n_s, n_e, n_d, steps),
        out_shape=(
            pltpu.VMEM((1, steps, tok_rows, width), BF),
            pltpu.VMEM((1, units, cols), F32),
        ),
        in_specs=[hbm] * 9,
        out_specs=(held, held),
        scratch_shapes=[
            vmem(CORES * n_d, units, cols),
            vmem(CORES * n_d, 2, units, sub),
            vmem(CORES * n_d, 2, units, sub),
            vmem(1, routes.shape[3], steps, tok_rows, kind=jnp.int32),
            vmem(1, routes.shape[3], steps, tok_rows),
            vmem(1, width, kind=F32),
            vmem(*cotangent.shape),
            vmem(tok_rows, width),
            vmem(steps, tok_rows, width),
            vmem(tok_rows, width),
            vmem(steps, n_c, flight, 8, packed),
            vmem(steps, n_c, n_y, 8, packed),
            vmem(steps, n_c, flight, 8, packed),
            vmem(steps, n_c, n_y, 8, packed),
            vmem(steps, CORES, n_d, 2, n_y, 8, packed),
            vmem(n_c, rows, sub),
            vmem(2, CORES, rows, units, kind=F32),
            vmem(steps, CORES, rows, units),
            vmem(steps, CORES * n_d, rows, units),
            vmem(CORES, 24 * n_y, units),
            vmem(steps, n_c, n_y, 8, packed),
            vmem(steps, n_c, n_y, 8, packed),
            vmem(used, tok_rows),
            vmem(used, tok_rows),
            vmem(n_c, tok_rows, sub),
            dma((11,)),
            dma((3,)),
            dma((5,)),
            dma((2, 11)),
            dma((SENDS,)),
            dma((SEMS,)),
            pltpu.SemaphoreType.REGULAR((READY,)),
        ],
        compiler_params=pltpu.CompilerParams(
            collective_id=0, has_side_effects=True, vmem_limit_bytes=64240 * 1024
        ),
    )(
        arrivals, fresh, jnp.transpose(routes, (0, 3, 1, 2)),
        jnp.transpose(gates, (0, 3, 1, 2)), cotangent,
        norm_gain, w_gate, w_up, w_down,
    )
    return pl.pallas_call(
        finish,
        out_shape=tuple(jax.ShapeDtypeStruct(m.shape, m.dtype) for m in made),
        in_specs=[held] * 2,
        out_specs=(hbm, hbm),
        scratch_shapes=[pltpu.SemaphoreType.DMA((2,))],
        compiler_params=pltpu.CompilerParams(vmem_limit_bytes=4096 * 1024),
    )(*made)


def solution(mesh):
    placed = (
        P("section", ("expert", "dp"), None),
        P(None, ("expert", "dp"), None),
        P("section", None, ("expert", "dp"), None),
        P("section", None, ("expert", "dp"), None),
        P("section", None, ("expert", "dp"), None),
        P("section", None),
        P("section", "expert", "dp"),
        P("section", "expert", "dp"),
        P("section", "expert", "dp"),
    )
    sizes = (mesh.shape["section"], mesh.shape["expert"], mesh.shape["dp"])
    return jax.shard_map(
        functools.partial(local, sizes),
        mesh=mesh,
        in_specs=placed,
        out_specs=(P("section", None, ("expert", "dp"), None), P("section", "expert", "dp")),
        check_vma=False,
    )
```
